32 devices in a mesh: row: 8 (over z, core), col: 4 (over y, x).
Axes of the slice: x: 2, y: 2, z: 4, core: 2. Of those that a mesh axis runs over, the one named last changes fastest.
Arguments:
- embedding: bfloat16 [256, 128], P('col'), may hold values from -6 to 6
- dilation: int32 [2], replicated, may hold values from 1 to 4, as said below
- kernel: bfloat16 [3, 3, 48, 128], replicated, may hold values from -0.1875 to 0.1875
- kernel_bias: float32 [48], replicated, may hold values from -3 to 3
- mixing: bfloat16 [5, 48], replicated, may hold values from -0.875 to 0.875
- mixing_bias: float32 [5], replicated, may hold values from -3 to 3
- cotangent: bfloat16 [5, 256, 256], P(None, 'row', 'col'), may hold values from -0.375 to 0.375
Outputs:
- contact: float32 [5, 256, 256], P(None, 'row', 'col')
- embedding_grad: float32 [256, 128], P('col')
- kernel_grad: float32 [3, 3, 48, 128], replicated
The draws below stay inside these ranges and needn't reach their ends.
Inputs may be any that keep to these rules, and one draw needn't show every extreme that they name: `dilation`: the larger of the two rates is exactly 4.
All inputs are finite; a program needn't handle non-finite values.
Results may differ from the reference program's by a relative error of at most 0.019.
The reference program's roundings to bfloat16 on the way count: a program that leaves them out, or rounds other values in their place, can miss the bound.
Values may be sent and summed in bfloat16 or wider, within the bound.
No kernel may reach another device: no remote copies, remote signals or barrier semaphores. Data moves between devices by JAX's collectives and lax.ppermute only.
A program may use at most 64 MiB of HBM per device.

```python
import jax
import jax.numpy as jnp
from jax import lax

C = 128
F = 48
NT = 5
DMAX = 4
BINS = 256
RB = 32
N_ROW = 8


def draw_dilation(key, part):
    first_key, second_key = jax.random.split(jax.random.fold_in(key, 11))
    larger_slot = jax.random.randint(first_key, (), 0, 2)
    other_rate = jax.random.randint(second_key, (), 1, DMAX + 1)
    slot_index = jnp.arange(2)
    return jnp.where(slot_index == larger_slot, DMAX, other_rate).astype(jnp.int32)


def block_scale(stream_key, shape, shards, low, high):
    factor_of, own = 1.0, jax.random.fold_in(stream_key, 6)
    for dim, shards_of in shards:
        steps = jnp.exp(jax.random.uniform(jax.random.fold_in(own, dim), (shards_of,), jnp.float32, low / len(shards), high / len(shards)))
        factor_of = factor_of * jnp.repeat(steps, shape[dim] // shards_of).reshape([-1 if axis == dim else 1 for axis in range(len(shape))])
    return factor_of


def normal_values(own_key, dims, spread, most, shards=(), kind=jnp.bfloat16):
    array = spread * jax.random.normal(own_key, dims, jnp.float32)
    if shards:
        array = array * block_scale(own_key, dims, shards, -0.22, 0.18)
    return jnp.clip(array, -most, most).astype(kind)


def setup_inputs(seed: int = 0) -> dict:
    splits = jax.random.split(jax.random.key(seed), 8)
    return {
        "embedding": normal_values(splits[0], (BINS, C), 1.0, 6.0, ((0, 4),)),
        "dilation": draw_dilation(jax.random.fold_in(splits[7], 71), 0),
        "kernel": normal_values(splits[2], (3, 3, F, C), (9 * C) ** -0.5, 0.1875),
        "kernel_bias": normal_values(splits[3], (F,), 0.5, 3.0, (), jnp.float32),
        "mixing": normal_values(splits[4], (NT, F), F ** -0.5, 0.875),
        "mixing_bias": normal_values(splits[5], (NT,), 0.5, 3.0, (), jnp.float32),
        "cotangent": normal_values(splits[6], (NT, BINS, BINS), 0.0625, 0.375, ((1, 8), (2, 4))),
    }


def tap_list():
    return [(tap_row, tap_col) for tap_row in (-1, 0, 1) for tap_col in (-1, 0, 1)]


def tap_anchor(tap_row, tap_col, row_rate, col_rate, mirrored):
    if mirrored:
        return DMAX + tap_col * col_rate, DMAX + tap_row * row_rate
    return DMAX + tap_row * row_rate, DMAX + tap_col * col_rate


def narrow(values):
    return lax.optimization_barrier(values.astype(jnp.bfloat16)).astype(jnp.float32)


def add_into(target, position, update):
    current = lax.dynamic_slice_in_dim(target, position, update.shape[0], 0)
    return lax.dynamic_update_slice_in_dim(target, current + update, position, 0)


def reference(embedding, dilation, kernel, kernel_bias, mixing, mixing_bias, cotangent):
    highest = lax.Precision.HIGHEST
    row_rate = dilation[0].astype(jnp.int32)
    col_rate = dilation[1].astype(jnp.int32)
    padded_len = BINS + 2 * DMAX
    padded = jnp.pad(embedding.astype(jnp.float32), ((DMAX, DMAX), (0, 0)))
    places = jnp.arange(padded_len, dtype=jnp.int32) - DMAX
    inside = ((places >= 0) & (places < BINS)).astype(jnp.float32)
    weights = kernel.astype(jnp.float32)
    mix_weights = mixing.astype(jnp.float32)
    zero_index = jnp.zeros((), jnp.int32)

    def block_step(running_sums, block_index):
        kernel_acc, row_acc, col_acc = running_sums
        block_start = block_index * RB
        row_values = lax.dynamic_slice_in_dim(padded, block_start, RB + 2 * DMAX, 0)
        row_inside = lax.dynamic_slice_in_dim(inside, block_start, RB + 2 * DMAX, 0)
        pairs = narrow(0.5 * (row_values[:, None, :] + padded[None, :, :]))
        pairs = pairs * (row_inside[:, None] * inside[None, :])[:, :, None]

        def slicer(tap_row, tap_col, mirrored):
            anchor = tap_anchor(tap_row, tap_col, row_rate, col_rate, mirrored)
            return lax.dynamic_slice(pairs, (anchor[0], anchor[1], zero_index), (RB, BINS, C))

        def convolve(mirrored):
            running = jnp.zeros((F, RB, BINS), jnp.float32)
            for tap_row, tap_col in tap_list():
                tap_piece = slicer(tap_row, tap_col, mirrored)
                running = running + jnp.einsum("ijc,fc->fij", tap_piece, weights[tap_row + 1, tap_col + 1], precision=highest)
            return running + kernel_bias[:, None, None]

        direct = convolve(False)
        mirror = convolve(True)
        direct_act = narrow(jax.nn.relu(direct))
        mirror_act = narrow(jax.nn.relu(mirror))

        def mix_map(activation):
            return jnp.einsum("tf,fij->tij", mix_weights, activation, precision=highest) + mixing_bias[:, None, None]

        contact_block = 0.5 * mix_map(direct_act) + 0.5 * mix_map(mirror_act)
        target = lax.dynamic_slice_in_dim(cotangent, block_start, RB, 1).astype(jnp.float32)
        guide_grad = narrow(0.5 * jnp.einsum("tf,tij->fij", mix_weights, target, precision=highest))
        grad_direct = jnp.where(direct > 0, guide_grad, jnp.zeros_like(guide_grad))
        grad_mirror = jnp.where(mirror > 0, guide_grad, jnp.zeros_like(guide_grad))

        updates = []
        for tap_row, tap_col in tap_list():
            tap_term = jnp.einsum("fij,ijc->fc", grad_direct, slicer(tap_row, tap_col, False), precision=highest)
            tap_term = tap_term + jnp.einsum("fij,ijc->fc", grad_mirror, slicer(tap_row, tap_col, True), precision=highest)
            updates.append(tap_term)
        kernel_acc = kernel_acc + jnp.stack(updates).reshape(3, 3, F, C)

        def col_mask(shift):
            return lax.dynamic_slice_in_dim(inside, DMAX + shift, BINS, 0)

        def row_mask(shift):
            return lax.dynamic_slice_in_dim(row_inside, DMAX + shift, RB, 0)

        direct_rows = [jnp.einsum("fij,j->fi", grad_direct, col_mask(tap_step * col_rate), precision=highest) for tap_step in (-1, 0, 1)]
        direct_cols = [jnp.einsum("fij,i->fj", grad_direct, row_mask(tap_step * row_rate), precision=highest) for tap_step in (-1, 0, 1)]
        mirror_rows = [jnp.einsum("fij,j->fi", grad_mirror, col_mask(tap_step * row_rate), precision=highest) for tap_step in (-1, 0, 1)]
        mirror_cols = [jnp.einsum("fij,i->fj", grad_mirror, row_mask(tap_step * col_rate), precision=highest) for tap_step in (-1, 0, 1)]
        for tap_row, tap_col in tap_list():
            tap_weight = weights[tap_row + 1, tap_col + 1]
            row_acc = add_into(row_acc, block_start + DMAX + tap_row * row_rate, jnp.einsum("fi,fc->ic", direct_rows[tap_col + 1], tap_weight, precision=highest))
            row_acc = add_into(row_acc, block_start + DMAX + tap_col * col_rate, jnp.einsum("fi,fc->ic", mirror_rows[tap_row + 1], tap_weight, precision=highest))
            col_acc = add_into(col_acc, DMAX + tap_col * col_rate, jnp.einsum("fj,fc->jc", direct_cols[tap_row + 1], tap_weight, precision=highest))
            col_acc = add_into(col_acc, DMAX + tap_row * row_rate, jnp.einsum("fj,fc->jc", mirror_cols[tap_col + 1], tap_weight, precision=highest))
        return (kernel_acc, row_acc, col_acc), contact_block

    initial = (jnp.zeros((3, 3, F, C), jnp.float32), jnp.zeros((padded_len, C), jnp.float32), jnp.zeros((padded_len, C), jnp.float32))
    finals, blocks = lax.scan(block_step, initial, jnp.arange(N_ROW, dtype=jnp.int32))
    kernel_grad, row_acc, col_acc = finals
    contact = jnp.transpose(blocks, (1, 0, 2, 3)).reshape(NT, BINS, BINS)
    embedding_grad = 0.5 * row_acc[DMAX:DMAX + BINS] + 0.5 * col_acc[DMAX:DMAX + BINS]
    return contact, embedding_grad, kernel_grad
```

```python
import functools

import jax
import jax.numpy as jnp
from jax import lax
from jax.experimental import pallas as pl
from jax.experimental.pallas import tpu as pltpu
from jax.sharding import PartitionSpec as P

DMAX = 4
PAD = 8
STEPS = (-1, 0, 1)
LANES = 128


def contract(left, right, dims):
    return lax.dot_general(left, right, (dims, ((), ())), preferred_element_type=jnp.float32)


def local_kernel(
    sizes,
    dilation_ref,
    *refs,
):
    peers, rows, cols, bins, filters, half = sizes
    block_refs = refs[:peers]
    kernel_ref, bias_ref, mix_ref, mix_bias_ref, cot_ref = refs[peers : peers + 5]
    contact_ref, send_ref, keep_ref = refs[peers + 5 : peers + 8]
    bins_ref, x_ref, weight_ref, grad_ref, wide_ref, acc_ref, taps_ref = refs[peers + 8 :]
    row_rate = dilation_ref[0]
    col_rate = dilation_ref[1]
    row_index = lax.axis_index("row")
    col_index = lax.axis_index("col")
    row_start = row_index * rows
    col_start = col_index * cols
    core = lax.rem(row_index, 2)
    taps = [(a, b) for a in STEPS for b in STEPS]
    count = len(taps)
    mirror_lane = LANES // 2
    bf16 = jnp.bfloat16
    f32 = jnp.float32

    bins_ref[0:PAD, :] = jnp.zeros((PAD, LANES), f32)
    bins_ref[bins + PAD : bins + 2 * PAD, :] = jnp.zeros((PAD, LANES), f32)
    for step in range(peers):
        place = pl.multiple_of(jnp.bitwise_xor(col_index, step) * cols + PAD, 8)
        bins_ref[pl.ds(place, cols), :] = 0.5 * block_refs[step][...].astype(f32)

    weight_ref[...] = jnp.zeros_like(weight_ref)
    wide_ref[...] = jnp.zeros_like(wide_ref)
    for at, (a, b) in enumerate(taps):
        tap = kernel_ref[at]
        weight_ref[0:filters, at * LANES : (at + 1) * LANES] = tap
        weight_ref[mirror_lane : mirror_lane + filters, (count + at) * LANES : (count + at + 1) * LANES] = tap
        first = (b + 1) * LANES
        wide_ref[first : first + filters, (a + 1) * LANES : (a + 2) * LANES] = tap
        first = (a + 1) * LANES + mirror_lane
        wide_ref[first : first + filters, (b + 4) * LANES : (b + 5) * LANES] = tap

    col_lane = lax.broadcasted_iota(jnp.int32, (cols, LANES), 0) + col_start

    def col_values(shift):
        values = bins_ref[pl.ds(col_start + PAD + shift, cols), :]
        place = col_lane + shift
        keep = ((place >= 0) & (place < bins)).astype(f32)
        return values, keep

    for at in range(2 * count):
        mirrored = at >= count
        a, b = taps[at % count]
        row_shift = b * col_rate if mirrored else a * row_rate
        col_shift = a * row_rate if mirrored else b * col_rate
        values, keep = col_values(col_shift)
        for i in range(rows):
            row = bins_ref[pl.ds(row_start + PAD + row_shift + i, 1), :]
            piece = (row + values) * keep
            if i < DMAX or i >= rows - DMAX:
                place = row_start + row_shift + i
                inside = (place >= 0) & (place < bins)
                piece = piece * inside.astype(f32)
            x_ref[i * cols : (i + 1) * cols, at * LANES : (at + 1) * LANES] = piece.astype(bf16)

    conv = contract(x_ref[...], weight_ref[...], ((1,), (1,))) + bias_ref[...]
    guide = contract(cot_ref[...], mix_ref[...], ((0,), (0,))).astype(bf16)
    grad = jnp.where(conv > 0, guide.astype(f32), 0.0)
    grad_ref[...] = grad
    active = jnp.maximum(conv, 0.0).astype(bf16)
    mixed = contract(mix_ref[...], active, ((1,), (1,)))
    contact_ref[...] = mixed[0:8] + mix_bias_ref[...]

    grad16 = grad.astype(bf16)
    turned = grad16.T
    kernel_terms = contract(turned[0:filters], x_ref[:, : count * LANES], ((1,), (0,)))
    kernel_terms = kernel_terms + contract(
        turned[mirror_lane : mirror_lane + filters], x_ref[:, count * LANES :], ((1,), (0,))
    )
    for at in range(count):
        taps_ref[at * filters : (at + 1) * filters, :] = kernel_terms[:, at * LANES : (at + 1) * LANES]

    is_mirror = lax.broadcasted_iota(jnp.int32, (1, LANES), 1) >= mirror_lane
    row_sums = []
    col_sums = []
    for q in STEPS:
        place = col_lane + jnp.where(is_mirror, q * row_rate, q * col_rate)
        keep = ((place >= 0) & (place < bins)).astype(f32)
        sums = [
            jnp.sum(grad_ref[i * cols : (i + 1) * cols, :] * keep, axis=0, keepdims=True)
            for i in range(rows)
        ]
        row_sums.append(jnp.concatenate(sums, axis=0))
        total = None
        for i in range(rows):
            place = row_start + i + jnp.where(is_mirror, q * col_rate, q * row_rate)
            keep = ((place >= 0) & (place < bins)).astype(f32)
            term = grad_ref[i * cols : (i + 1) * cols, :] * keep
            total = term if total is None else total + term
        col_sums.append(pltpu.roll(total, mirror_lane, 1))
    sums = jnp.concatenate(
        [jnp.concatenate(row_sums, axis=1), jnp.concatenate(col_sums, axis=1)], axis=0
    ).astype(bf16)
    spread = contract(sums, wide_ref[...], ((1,), (0,)))
    acc_ref[...] = jnp.zeros_like(acc_ref)
    for group in range(6):
        shift = STEPS[group % 3] * (row_rate if group < 3 else col_rate)
        piece = spread[:, group * LANES : (group + 1) * LANES]
        where = pl.ds(row_start + PAD + shift, rows)
        acc_ref[where, :] = acc_ref[where, :] + piece[0:rows]
        where = pl.ds(col_start + PAD + shift, cols)
        acc_ref[where, :] = acc_ref[where, :] + piece[rows : rows + cols]

    total_rows = count * filters
    for target, which in ((keep_ref, core), (send_ref, 1 - core)):
        first = pl.multiple_of(which * (total_rows - half), 16)
        target[0:half, :] = taps_ref[pl.ds(first, half), :].astype(bf16)
        part = cols // 2
        for step in range(peers):
            first = pl.multiple_of(which * part + (step * cols + PAD), 8)
            target[half + step * part : half + (step + 1) * part, :] = (
                0.5 * acc_ref[pl.ds(first, part), :]
            ).astype(bf16)


def swap(value, axis, mask):
    peers = lax.axis_size(axis)
    return lax.ppermute(value, axis, [(i, i ^ mask) for i in range(peers)])


def per_device(embedding, dilation, kernel, kernel_bias, mixing, mixing_bias, cotangent):
    f32 = jnp.float32
    bf16 = jnp.bfloat16
    filters, channels = kernel.shape[2:]
    maps, rows, cols = cotangent.shape
    peers = lax.axis_size("col")
    row_peers = lax.axis_size("row")
    bins = cols * peers
    core = lax.rem(lax.axis_index("row"), 2)
    col_index = lax.axis_index("col")
    blocks = [embedding] + [swap(embedding, "col", mask) for mask in range(1, peers)]
    spare = LANES // 2 - filters
    taps = 9
    taps_rows = taps * filters
    half = (taps_rows // 2 + 15) // 16 * 16

    def twice(value):
        wide = jnp.pad(value, ((0, 0), (0, spare)))
        return jnp.concatenate([wide, wide], axis=1)

    bias = twice(kernel_bias[None, :])
    mix = jnp.pad(twice(0.5 * mixing), ((0, 16 - maps), (0, 0))).astype(bf16)
    mix_bias = jnp.pad(mixing_bias, (0, 8 - maps))[:, None]
    cot = jnp.pad(cotangent.reshape(maps, rows * cols), ((0, 16 - maps), (0, 0)))
    packed = half + peers * cols // 2
    vmem = pl.BlockSpec(memory_space=pltpu.VMEM)
    contact, send, keep = pl.pallas_call(
        functools.partial(local_kernel, (peers, rows, cols, bins, filters, half)),
        out_shape=(
            jax.ShapeDtypeStruct((8, rows * cols), f32),
            jax.ShapeDtypeStruct((packed, LANES), bf16),
            jax.ShapeDtypeStruct((packed, LANES), bf16),
        ),
        in_specs=[pl.BlockSpec(memory_space=pltpu.SMEM)] + [vmem] * (peers + 5),
        out_specs=(vmem, vmem, vmem),
        scratch_shapes=[
            pltpu.VMEM((bins + 2 * PAD, LANES), f32),
            pltpu.VMEM((rows * cols, 2 * taps * LANES), bf16),
            pltpu.VMEM((LANES, 2 * taps * LANES), bf16),
            pltpu.VMEM((rows * cols, LANES), f32),
            pltpu.VMEM((3 * LANES, 6 * LANES), bf16),
            pltpu.VMEM((bins + 2 * PAD, LANES), f32),
            pltpu.VMEM((taps_rows, LANES), f32),
        ],
        name="contact_head",
    )(dilation, *blocks, kernel.reshape(taps, filters, channels), bias, mix, mix_bias, cot)

    total = keep + swap(send, "row", 1)
    mask = 1
    while mask < peers:
        total = total + swap(total, "col", mask)
        mask *= 2
    mask = 2
    while mask < row_peers:
        total = total + swap(total, "row", mask)
        mask *= 2
    part = cols // 2
    mine = lax.dynamic_slice_in_dim(total[half:], col_index * part, part, 0)
    mine = jnp.concatenate([total[:half], mine], axis=0)
    other = swap(mine, "row", 1)
    low = jnp.where(core == 0, mine, other).astype(f32)
    high = jnp.where(core == 0, other, mine).astype(f32)
    kernel_grad = jnp.concatenate([low[: taps_rows - half], high[:half]], axis=0)
    embedding_grad = jnp.concatenate([low[half:], high[half:]], axis=0)
    return (
        contact[:maps].reshape(maps, rows, cols),
        embedding_grad,
        kernel_grad.reshape(kernel.shape),
    )


def solution(mesh):
    return jax.shard_map(
        per_device,
        mesh=mesh,
        in_specs=(P("col", None), P(), P(), P(), P(), P(), P(None, "row", "col")),
        out_specs=(P(None, "row", "col"), P("col", None), P()),
        check_vma=False,
    )
```

```python
import functools

import jax
import jax.numpy as jnp
from jax import lax
from jax.experimental import pallas as pl
from jax.experimental.pallas import tpu as pltpu
from jax.sharding import PartitionSpec as P

DMAX = 4
PAD = 8
STEPS = (-1, 0, 1)
LANES = 128


def contract(left, right, dims):
    return lax.dot_general(left, right, (dims, ((), ())), preferred_element_type=jnp.float32)


def local_kernel(
    sizes,
    dilation_ref,
    *refs,
):
    peers, rows, cols, bins, filters, half = sizes
    block_refs = refs[:peers]
    kernel_ref, bias_ref, mix_ref, mix_bias_ref, cot_ref = refs[peers : peers + 5]
    contact_ref, send_ref, keep_ref = refs[peers + 5 : peers + 8]
    bins_ref, x_ref, weight_ref, grad_ref, wide_ref, acc_ref, taps_ref = refs[peers + 8 :]
    row_rate = dilation_ref[0]
    col_rate = dilation_ref[1]
    row_index = lax.axis_index("row")
    col_index = lax.axis_index("col")
    row_start = row_index * rows
    col_start = col_index * cols
    core = lax.rem(row_index, 2)
    taps = [(a, b) for a in STEPS for b in STEPS]
    count = len(taps)
    mirror_lane = LANES // 2
    bf16 = jnp.bfloat16
    f32 = jnp.float32

    bins_ref[0:PAD, :] = jnp.zeros((PAD, LANES), f32)
    bins_ref[bins + PAD : bins + 2 * PAD, :] = jnp.zeros((PAD, LANES), f32)
    for step in range(peers):
        place = pl.multiple_of(jnp.bitwise_xor(col_index, step) * cols + PAD, 8)
        bins_ref[pl.ds(place, cols), :] = 0.5 * block_refs[step][...].astype(f32)

    weight_ref[...] = jnp.zeros_like(weight_ref)
    wide_ref[...] = jnp.zeros_like(wide_ref)
    for at, (a, b) in enumerate(taps):
        tap = kernel_ref[at]
        weight_ref[0:filters, at * LANES : (at + 1) * LANES] = tap
        weight_ref[mirror_lane : mirror_lane + filters, (count + at) * LANES : (count + at + 1) * LANES] = tap
        first = (b + 1) * LANES
        wide_ref[first : first + filters, (a + 1) * LANES : (a + 2) * LANES] = tap
        first = (a + 1) * LANES + mirror_lane
        wide_ref[first : first + filters, (b + 4) * LANES : (b + 5) * LANES] = tap

    col_lane = lax.broadcasted_iota(jnp.int32, (cols, LANES), 0) + col_start

    def col_values(shift):
        values = bins_ref[pl.ds(col_start + PAD + shift, cols), :]
        place = col_lane + shift
        keep = ((place >= 0) & (place < bins)).astype(f32)
        return values, keep

    for at in range(2 * count):
        mirrored = at >= count
        a, b = taps[at % count]
        row_shift = b * col_rate if mirrored else a * row_rate
        col_shift = a * row_rate if mirrored else b * col_rate
        values, keep = col_values(col_shift)
        for i in range(rows):
            row = bins_ref[pl.ds(row_start + PAD + row_shift + i, 1), :]
            piece = (row + values) * keep
            if i < DMAX or i >= rows - DMAX:
                place = row_start + row_shift + i
                inside = (place >= 0) & (place < bins)
                piece = piece * inside.astype(f32)
            x_ref[i * cols : (i + 1) * cols, at * LANES : (at + 1) * LANES] = piece.astype(bf16)

    conv = contract(x_ref[...], weight_ref[...], ((1,), (1,))) + bias_ref[...]
    guide = contract(cot_ref[...], mix_ref[...], ((0,), (0,))).astype(bf16)
    grad = jnp.where(conv > 0, guide.astype(f32), 0.0)
    grad_ref[...] = grad
    active = jnp.maximum(conv, 0.0).astype(bf16)
    mixed = contract(mix_ref[...], active, ((1,), (1,)))
    contact_ref[...] = mixed[0:8] + mix_bias_ref[...]

    grad16 = grad.astype(bf16)
    turned = grad16.T
    kernel_terms = contract(turned[0:filters], x_ref[:, : count * LANES], ((1,), (0,)))
    kernel_terms = kernel_terms + contract(
        turned[mirror_lane : mirror_lane + filters], x_ref[:, count * LANES :], ((1,), (0,))
    )
    for at in range(count):
        taps_ref[at * filters : (at + 1) * filters, :] = kernel_terms[:, at * LANES : (at + 1) * LANES]

    is_mirror = lax.broadcasted_iota(jnp.int32, (1, LANES), 1) >= mirror_lane
    row_sums = []
    col_sums = []
    for q in STEPS:
        place = col_lane + jnp.where(is_mirror, q * row_rate, q * col_rate)
        keep = ((place >= 0) & (place < bins)).astype(f32)
        sums = [
            jnp.sum(grad_ref[i * cols : (i + 1) * cols, :] * keep, axis=0, keepdims=True)
            for i in range(rows)
        ]
        row_sums.append(jnp.concatenate(sums, axis=0))
        total = None
        for i in range(rows):
            place = row_start + i + jnp.where(is_mirror, q * col_rate, q * row_rate)
            keep = ((place >= 0) & (place < bins)).astype(f32)
            term = grad_ref[i * cols : (i + 1) * cols, :] * keep
            total = term if total is None else total + term
        col_sums.append(pltpu.roll(total, mirror_lane, 1))
    sums = jnp.concatenate(
        [jnp.concatenate(row_sums, axis=1), jnp.concatenate(col_sums, axis=1)], axis=0
    ).astype(bf16)
    spread = contract(sums, wide_ref[...], ((1,), (0,)))
    acc_ref[...] = jnp.zeros_like(acc_ref)
    for group in range(6):
        shift = STEPS[group % 3] * (row_rate if group < 3 else col_rate)
        piece = spread[:, group * LANES : (group + 1) * LANES]
        where = pl.ds(row_start + PAD + shift, rows)
        acc_ref[where, :] = acc_ref[where, :] + piece[0:rows]
        where = pl.ds(col_start + PAD + shift, cols)
        acc_ref[where, :] = acc_ref[where, :] + piece[rows : rows + cols]

    total_rows = count * filters
    for target, which in ((keep_ref, core), (send_ref, 1 - core)):
        first = pl.multiple_of(which * (total_rows - half), 16)
        target[0:half, :] = taps_ref[pl.ds(first, half), :].astype(bf16)
        part = cols // 2
        for step in range(peers):
            first = pl.multiple_of(which * part + (step * cols + PAD), 8)
            target[half + step * part : half + (step + 1) * part, :] = (
                0.5 * acc_ref[pl.ds(first, part), :]
            ).astype(bf16)


def join_kernel(half, mine_ref, other_ref, embedding_ref, taps_ref):
    core = lax.rem(lax.axis_index("row"), 2)
    total_rows = taps_ref.shape[0]
    part = embedding_ref.shape[0] // 2
    mine = mine_ref[...].astype(jnp.float32)
    other = other_ref[...].astype(jnp.float32)
    low = jnp.where(core == 0, mine, other)
    high = jnp.where(core == 0, other, mine)
    taps_ref[0 : total_rows - half, :] = low[0 : total_rows - half]
    taps_ref[total_rows - half : total_rows, :] = high[0:half]
    embedding_ref[0:part, :] = low[half : half + part]
    embedding_ref[part : 2 * part, :] = high[half : half + part]


def swap(value, axis, mask):
    peers = lax.axis_size(axis)
    return lax.ppermute(value, axis, [(i, i ^ mask) for i in range(peers)])


def per_device(embedding, dilation, kernel, kernel_bias, mixing, mixing_bias, cotangent):
    f32 = jnp.float32
    bf16 = jnp.bfloat16
    filters, channels = kernel.shape[2:]
    maps, rows, cols = cotangent.shape
    peers = lax.axis_size("col")
    row_peers = lax.axis_size("row")
    bins = cols * peers
    col_index = lax.axis_index("col")
    blocks = [embedding] + [swap(embedding, "col", mask) for mask in range(1, peers)]
    spare = LANES // 2 - filters
    taps = 9
    taps_rows = taps * filters
    half = (taps_rows // 2 + 15) // 16 * 16

    def twice(value):
        wide = jnp.pad(value, ((0, 0), (0, spare)))
        return jnp.concatenate([wide, wide], axis=1)

    bias = twice(kernel_bias[None, :])
    mix = jnp.pad(twice(0.5 * mixing), ((0, 16 - maps), (0, 0))).astype(bf16)
    mix_bias = jnp.pad(mixing_bias, (0, 8 - maps))[:, None]
    cot = jnp.pad(cotangent.reshape(maps, rows * cols), ((0, 16 - maps), (0, 0)))
    packed = half + peers * cols // 2
    vmem = pl.BlockSpec(memory_space=pltpu.VMEM)
    contact, send, keep = pl.pallas_call(
        functools.partial(local_kernel, (peers, rows, cols, bins, filters, half)),
        out_shape=(
            jax.ShapeDtypeStruct((8, rows * cols), f32),
            jax.ShapeDtypeStruct((packed, LANES), bf16),
            jax.ShapeDtypeStruct((packed, LANES), bf16),
        ),
        in_specs=[pl.BlockSpec(memory_space=pltpu.SMEM)] + [vmem] * (peers + 5),
        out_specs=(vmem, vmem, vmem),
        scratch_shapes=[
            pltpu.VMEM((bins + 2 * PAD, LANES), f32),
            pltpu.VMEM((rows * cols, 2 * taps * LANES), bf16),
            pltpu.VMEM((LANES, 2 * taps * LANES), bf16),
            pltpu.VMEM((rows * cols, LANES), f32),
            pltpu.VMEM((3 * LANES, 6 * LANES), bf16),
            pltpu.VMEM((bins + 2 * PAD, LANES), f32),
            pltpu.VMEM((taps_rows, LANES), f32),
        ],
        compiler_params=pltpu.CompilerParams(vmem_limit_bytes=24 * 1024 * 1024),
        name="contact_head",
    )(dilation, *blocks, kernel.reshape(taps, filters, channels), bias, mix, mix_bias, cot)

    total = keep + swap(send, "row", 1)
    mask = 1
    while mask < peers:
        total = total + swap(total, "col", mask)
        mask *= 2
    contact = contact[:maps].reshape(maps, rows, cols)
    total, contact = lax.optimization_barrier((total, contact))
    mask = 2
    while mask < row_peers:
        total = total + swap(total, "row", mask)
        mask *= 2
    part = cols // 2
    mine = lax.dynamic_slice_in_dim(total[half:], col_index * part, part, 0)
    mine = jnp.concatenate([total[:half], mine], axis=0)
    other = swap(mine, "row", 1)
    embedding_grad, kernel_grad = pl.pallas_call(
        functools.partial(join_kernel, half),
        out_shape=(
            jax.ShapeDtypeStruct((cols, channels), f32),
            jax.ShapeDtypeStruct((taps_rows, channels), f32),
        ),
        in_specs=[vmem, vmem],
        out_specs=(vmem, vmem),
        compiler_params=pltpu.CompilerParams(vmem_limit_bytes=4 * 1024 * 1024),
        name="join",
    )(mine, other)
    return contact, embedding_grad, kernel_grad.reshape(kernel.shape)


def solution(mesh):
    return jax.shard_map(
        per_device,
        mesh=mesh,
        in_specs=(P("col", None), P(), P(), P(), P(), P(), P(None, "row", "col")),
        out_specs=(P(None, "row", "col"), P("col", None), P()),
        check_vma=False,
    )
```

```python
import functools

import jax
import jax.numpy as jnp
from jax import lax
from jax.experimental import pallas as pl
from jax.experimental.pallas import tpu as pltpu
from jax.sharding import PartitionSpec as P

DMAX = 4
PAD = 8
STEPS = (-1, 0, 1)
TAPS = [(a, b) for a in STEPS for b in STEPS]
LANES = 128
HALF = LANES // 2


def contract(left, right, dims):
    return lax.dot_general(left, right, (dims, ((), ())), preferred_element_type=jnp.float32)


def prepare_kernel(
    embedding_hbm,
    dilation_hbm,
    kernel_hbm,
    bias_hbm,
    mixing_hbm,
    cot_hbm,
    own_ref,
    rate_ref,
    weight_ref,
    wide_ref,
    guide_ref,
    mix_ref,
    wide_bias_ref,
    rates,
    kernel_ref,
    bias_ref,
    mixing_ref,
    cot_ref,
    flat_ref,
    semaphores,
):
    pairs = (
        (kernel_hbm, kernel_ref),
        (cot_hbm, cot_ref),
        (mixing_hbm, mixing_ref),
        (bias_hbm, bias_ref),
        (dilation_hbm, rates),
        (embedding_hbm, own_ref),
    )
    copies = [pltpu.make_async_copy(*pair, semaphores.at[at]) for at, pair in enumerate(pairs)]
    for copy in copies:
        copy.start()
    filters = kernel_ref.shape[1]
    maps, rows, cols = cot_ref.shape
    weight_ref[...] = jnp.zeros_like(weight_ref)
    wide_ref[...] = jnp.zeros_like(wide_ref)
    wide_bias_ref[...] = jnp.zeros_like(wide_bias_ref)
    for copy in copies:
        copy.wait()
    lead = (0, HALF, 2 * HALF)
    side = (HALF, 0, 3 * HALF)
    for at, (a, b) in enumerate(TAPS):
        tap = kernel_ref[at]
        first = lead[a + 1]
        weight_ref[0, first : first + filters, (b + 1) * LANES : (b + 2) * LANES] = tap
        first = side[b + 1]
        weight_ref[1, first : first + filters, (a + 1) * LANES : (a + 2) * LANES] = tap
        first = (b + 1) * LANES
        wide_ref[first : first + filters, (a + 1) * LANES : (a + 2) * LANES] = tap
        first = (a + 1) * LANES + HALF
        wide_ref[first : first + filters, (b + 4) * LANES : (b + 5) * LANES] = tap
    rate_ref[0:8, :] = jnp.full((8, LANES), rates[0], jnp.int32)
    rate_ref[8:16, :] = jnp.full((8, LANES), rates[1], jnp.int32)
    wide_bias_ref[0:1, 0:filters] = bias_ref[...]
    wide_bias_ref[0:1, HALF : HALF + filters] = bias_ref[...]
    mix = 0.5 * mixing_ref[...].astype(jnp.float32)
    spare = jnp.zeros((maps, HALF - filters), jnp.float32)
    mix = jnp.concatenate([mix, spare, mix, spare], axis=1)
    mix_ref[0:maps, :] = mix
    mix_ref[maps:16, :] = jnp.zeros((16 - maps, LANES), jnp.float32)
    for t in range(maps):
        flat_ref[t * rows : (t + 1) * rows, :] = cot_ref[t].astype(jnp.float32)
    lines = [flat_ref[pl.ds(i, maps, stride=rows), :] for i in range(rows)]
    cot = jnp.concatenate(lines, axis=1).astype(jnp.bfloat16)
    mix = mix.astype(jnp.bfloat16)
    guide_ref[...] = contract(cot, mix, ((0,), (0,))).astype(jnp.bfloat16)


def contact_kernel(mix_bias_ref, mix_ref, active_ref, contact_ref):
    mix = mix_ref[...].astype(jnp.bfloat16)
    mixed = contract(mix, active_ref[...], ((1,), (1,)))
    maps = contact_ref.shape[0]
    which = lax.broadcasted_iota(jnp.int32, (8, 1), 0)
    offset = jnp.zeros((8, 1), jnp.float32)
    for t in range(maps):
        offset = jnp.where(which == t, mix_bias_ref[t], offset)
    contact_ref[...] = (mixed[0:8] + offset)[0:maps]


def local_kernel(sizes, *refs):
    peers, rows, cols, bins, filters, half = sizes
    block_refs = refs[:peers]
    rate_ref, weight_ref, wide_ref, guide_ref, bias_ref = refs[peers : peers + 5]
    active_ref, send_ref, keep_ref = refs[peers + 5 : peers + 8]
    bins_ref, pair_ref, conv_ref, grad_ref, turned_ref, acc_ref, taps_ref = refs[peers + 8 :]
    row_rate = jnp.max(rate_ref[0:8, :])
    col_rate = jnp.max(rate_ref[8:16, :])
    row_index = lax.axis_index("row")
    col_index = lax.axis_index("col")
    row_start = row_index * rows
    col_start = col_index * cols
    core = lax.rem(row_index, 2)
    count = len(TAPS)
    bf16 = jnp.bfloat16
    f32 = jnp.float32
    extended = rows + 2 * DMAX

    bins_ref[0:PAD, :] = jnp.zeros((PAD, LANES), f32)
    bins_ref[bins + PAD : bins + 2 * PAD, :] = jnp.zeros((PAD, LANES), f32)
    for step in range(peers):
        place = pl.multiple_of(jnp.bitwise_xor(col_index, step) * cols + PAD, 8)
        bins_ref[pl.ds(place, cols), :] = 0.5 * block_refs[step][...].astype(f32)

    col_place = lax.broadcasted_iota(jnp.int32, (cols, LANES), 0) + col_start
    edge = 16
    values = []
    keeps = []
    for shift in (0, -col_rate, col_rate, -row_rate, row_rate):
        values.append(bins_ref[pl.ds(col_start + PAD + shift, cols), :].astype(bf16))
        place = col_place + shift
        keeps.append(((place >= 0) & (place < bins)).astype(f32).astype(bf16))
    for m in range(extended):
        row = bins_ref[pl.ds(row_start + PAD - DMAX + m, 1), :]
        row = jnp.broadcast_to(row, (edge, LANES)).astype(bf16)
        place = row_start - DMAX + m
        inside = ((place >= 0) & (place < bins)).astype(f32).astype(bf16)
        for slot in range(5):
            for j in range(0, cols, edge):
                piece = row + values[slot][j : j + edge]
                if slot > 0 and (j == 0 or j + edge == cols):
                    piece = piece * keeps[slot][j : j + edge]
                if m < DMAX or m >= rows + DMAX:
                    piece = piece * inside
                pair_ref[slot, m * cols + j : m * cols + j + edge, :] = piece

    def shifted_columns(first, last):
        return jnp.concatenate([pair_ref[first], pair_ref[0], pair_ref[last]], axis=1)

    conv_ref[0] = contract(shifted_columns(1, 2), weight_ref[0], ((1,), (1,)))
    conv_ref[1] = contract(shifted_columns(3, 4), weight_ref[1], ((1,), (1,)))

    lane = lax.broadcasted_iota(jnp.int32, (1, LANES), 1)
    is_mirror = lane >= HALF
    bias = bias_ref[0:1, :]
    row_keeps = []
    for q in STEPS:
        place = col_place + jnp.where(is_mirror, q * row_rate, q * col_rate)
        row_keeps.append(((place >= 0) & (place < bins)).astype(f32))
    margin = PAD * cols
    grad_ref[0:margin, :] = jnp.zeros((margin, LANES), bf16)
    grad_ref[margin + rows * cols : 2 * margin + rows * cols, :] = jnp.zeros((margin, LANES), bf16)
    row_sums = [[], [], []]
    col_middle = None
    col_edges = [None, None, None]

    def add(total, term):
        return term if total is None else total + term

    for i in range(rows):
        def part(mirrored, shift, group):
            first = pl.multiple_of((DMAX + i + shift) * cols, cols)
            return conv_ref[mirrored, pl.ds(first, cols), group * LANES : (group + 1) * LANES]

        swapped = jnp.where(is_mirror, part(0, 0, 0), part(1, 0, 0))
        conv = jnp.where(is_mirror, part(1, -col_rate, 0), part(0, -row_rate, 0))
        conv = conv + pltpu.roll(swapped, HALF, 1)
        conv = conv + (part(0, row_rate, 1) + part(1, col_rate, 1))
        conv = conv + bias
        here = slice(i * cols, (i + 1) * cols)
        grad = jnp.where(conv > 0, guide_ref[here, :].astype(f32), 0.0)
        active_ref[here, :] = jnp.maximum(conv, 0.0).astype(bf16)
        grad_ref[margin + i * cols : margin + (i + 1) * cols, :] = grad.astype(bf16)
        last = cols - 8
        inner = grad[8:16]
        for j in range(16, last, 8):
            inner = inner + grad[j : j + 8]
        for q in range(3):
            keep = row_keeps[q]
            eight = inner + grad[0:8] * keep[0:8] + grad[last:cols] * keep[last:cols]
            row_sums[q].append(jnp.sum(eight, axis=0, keepdims=True))
            if i < DMAX or i >= rows - DMAX:
                step = STEPS[q]
                place = row_start + i + jnp.where(is_mirror, step * col_rate, step * row_rate)
                keep = ((place >= 0) & (place < bins)).astype(f32)
                col_edges[q] = add(col_edges[q], grad * keep)
        if DMAX <= i < rows - DMAX:
            col_middle = add(col_middle, grad)

    chunks = (2 * margin + rows * cols) // LANES
    first_chunk = margin // LANES
    last_chunk = chunks - first_chunk
    blank = jnp.zeros((LANES, LANES), bf16)
    for odd in range(2):
        for chunk in range(chunks):
            at = slice(chunk * LANES, (chunk + 1) * LANES)
            if first_chunk <= chunk < last_chunk + odd:
                begin = chunk * LANES - odd * cols
                turned_ref[odd, :, at] = grad_ref[begin : begin + LANES, :].T
            else:
                turned_ref[odd, :, at] = blank

    def shifted_rows(first, rate):
        pieces = []
        for q in STEPS:
            start = (DMAX - q * rate) * cols
            odd = lax.rem(lax.rem(q * rate, 2) + 2, 2)
            start = pl.multiple_of(start + odd * cols, LANES)
            pieces.append(turned_ref[odd, first : first + filters, pl.ds(start, extended * cols)])
        return jnp.concatenate(pieces, axis=0)

    direct = contract(shifted_rows(0, row_rate), shifted_columns(1, 2), ((1,), (0,)))
    mirror = contract(shifted_rows(HALF, col_rate), shifted_columns(3, 4), ((1,), (0,)))
    for at, (a, b) in enumerate(TAPS):
        a, b = a + 1, b + 1
        taps_ref[at * filters : (at + 1) * filters, :] = (
            direct[a * filters : (a + 1) * filters, b * LANES : (b + 1) * LANES]
            + mirror[b * filters : (b + 1) * filters, a * LANES : (a + 1) * LANES]
        )

    row_sums = [jnp.concatenate(sums, axis=0) for sums in row_sums]
    col_sums = [pltpu.roll(col_middle + edges, HALF, 1) for edges in col_edges]
    sums = jnp.concatenate(
        [jnp.concatenate(row_sums, axis=1), jnp.concatenate(col_sums, axis=1)], axis=0
    ).astype(bf16)
    spread = contract(sums, wide_ref[...], ((1,), (0,)))
    acc_ref[...] = jnp.zeros_like(acc_ref)
    for group in range(6):
        shift = STEPS[group % 3] * (row_rate if group < 3 else col_rate)
        piece = spread[:, group * LANES : (group + 1) * LANES]
        where = pl.ds(row_start + PAD + shift, rows)
        acc_ref[where, :] = acc_ref[where, :] + piece[0:rows]
        where = pl.ds(col_start + PAD + shift, cols)
        acc_ref[where, :] = acc_ref[where, :] + piece[rows : rows + cols]

    total_rows = count * filters
    for target, which in ((keep_ref, core), (send_ref, 1 - core)):
        first = pl.multiple_of(which * (total_rows - half), 16)
        target[0:half, :] = taps_ref[pl.ds(first, half), :].astype(bf16)
        part = cols // 2
        for step in range(peers):
            first = pl.multiple_of(which * part + (step * cols + PAD), 8)
            target[half + step * part : half + (step + 1) * part, :] = (
                0.5 * acc_ref[pl.ds(first, part), :]
            ).astype(bf16)


def join_kernel(half, mine_ref, other_ref, embedding_ref, taps_ref):
    core = lax.rem(lax.axis_index("row"), 2)
    total_rows = taps_ref.shape[0]
    part = embedding_ref.shape[0] // 2
    mine = mine_ref[...].astype(jnp.float32)
    other = other_ref[...].astype(jnp.float32)
    low = jnp.where(core == 0, mine, other)
    high = jnp.where(core == 0, other, mine)
    taps_ref[0 : total_rows - half, :] = low[0 : total_rows - half]
    taps_ref[total_rows - half : total_rows, :] = high[0:half]
    embedding_ref[0:part, :] = low[half : half + part]
    embedding_ref[part : 2 * part, :] = high[half : half + part]


def swap(value, axis, mask):
    peers = lax.axis_size(axis)
    return lax.ppermute(value, axis, [(i, i ^ mask) for i in range(peers)])


def per_device(embedding, dilation, kernel, kernel_bias, mixing, mixing_bias, cotangent):
    f32 = jnp.float32
    bf16 = jnp.bfloat16
    filters, channels = kernel.shape[2:]
    maps, rows, cols = cotangent.shape
    peers = lax.axis_size("col")
    row_peers = lax.axis_size("row")
    bins = cols * peers
    col_index = lax.axis_index("col")
    blocks = [embedding] + [swap(embedding, "col", mask) for mask in range(1, peers)]
    taps = len(TAPS)
    taps_rows = taps * filters
    half = (taps_rows // 2 + 15) // 16 * 16
    spots = rows * cols
    packed = half + peers * cols // 2
    vmem = pl.BlockSpec(memory_space=pltpu.VMEM)
    mib = 1024 * 1024

    def call(body, name, out_shape, inputs, scratch=(), limit=16, specs=None, flops=1000):
        return pl.pallas_call(
            body,
            out_shape=out_shape,
            in_specs=specs or [vmem] * len(inputs),
            out_specs=jax.tree.map(lambda _: vmem, out_shape),
            scratch_shapes=list(scratch),
            compiler_params=pltpu.CompilerParams(vmem_limit_bytes=limit * mib),
            cost_estimate=pl.CostEstimate(flops=flops, bytes_accessed=1000, transcendentals=0),
            name=name,
        )(*inputs)

    shape = jax.ShapeDtypeStruct
    kernels = kernel.reshape(taps, filters, channels)
    own, rates, weight, wide, guide, mix, bias = call(
        prepare_kernel,
        "prepare",
        (
            shape(embedding.shape, bf16),
            shape((16, LANES), jnp.int32),
            shape((2, 2 * LANES, 3 * LANES), bf16),
            shape((3 * LANES, 6 * LANES), bf16),
            shape((spots, LANES), bf16),
            shape((16, LANES), f32),
            shape((8, LANES), f32),
        ),
        (embedding, dilation, kernels, kernel_bias[None, :], mixing, cotangent),
        scratch=(
            pltpu.SMEM((2,), jnp.int32),
            pltpu.VMEM(kernels.shape, bf16),
            pltpu.VMEM((1, filters), f32),
            pltpu.VMEM(mixing.shape, bf16),
            pltpu.VMEM(cotangent.shape, bf16),
            pltpu.VMEM((maps * rows, cols), f32),
            pltpu.SemaphoreType.DMA((6,)),
        ),
        specs=[pl.BlockSpec(memory_space=pltpu.HBM)] * 6,
        flops=4_000_000_000,
    )
    blocks[0] = own
    extended = (rows + 2 * DMAX) * cols
    padded = spots + 2 * PAD * cols
    active, send, keep = call(
        functools.partial(local_kernel, (peers, rows, cols, bins, filters, half)),
        "contact_head",
        (shape((spots, LANES), bf16), shape((packed, LANES), bf16), shape((packed, LANES), bf16)),
        (*blocks, rates, weight, wide, guide, bias),
        scratch=(
            pltpu.VMEM((bins + 2 * PAD, LANES), f32),
            pltpu.VMEM((5, extended, LANES), bf16),
            pltpu.VMEM((2, extended, 2 * LANES), f32),
            pltpu.VMEM((padded, LANES), bf16),
            pltpu.VMEM((2, LANES, padded), bf16),
            pltpu.VMEM((bins + 2 * PAD, LANES), f32),
            pltpu.VMEM((taps_rows, LANES), f32),
        ),
        limit=24,
        flops=20_000_000_000,
    )

    total = keep + swap(send, "row", 1)
    mask = 1
    while mask < peers:
        total = total + swap(total, "col", mask)
        mask *= 2
    contact = call(
        contact_kernel,
        "contact",
        shape((maps, spots), f32),
        (mixing_bias, mix, active),
        specs=[pl.BlockSpec(memory_space=pltpu.SMEM), vmem, vmem],
        flops=1_000_000_000,
    ).reshape(maps, rows, cols)
    total, contact = lax.optimization_barrier((total, contact))
    mask = 2
    while mask < row_peers:
        total = total + swap(total, "row", mask)
        mask *= 2
    part = cols // 2
    mine = lax.dynamic_slice_in_dim(total[half:], col_index * part, part, 0)
    mine = jnp.concatenate([total[:half], mine], axis=0)
    other = swap(mine, "row", 1)
    embedding_grad, kernel_grad = call(
        functools.partial(join_kernel, half),
        "join",
        (shape((cols, channels), f32), shape((taps_rows, channels), f32)),
        (mine, other),
        limit=4,
    )
    return contact, embedding_grad, kernel_grad.reshape(kernel.shape)


def solution(mesh):
    return jax.shard_map(
        per_device,
        mesh=mesh,
        in_specs=(P("col", None), P(), P(), P(), P(), P(), P(None, "row", "col")),
        out_specs=(P(None, "row", "col"), P("col", None), P()),
        check_vma=False,
    )
```

```python
import functools

import jax
import jax.numpy as jnp
from jax import lax
from jax.experimental import pallas as pl
from jax.experimental.pallas import tpu as pltpu
from jax.sharding import PartitionSpec as P

DMAX = 4
PAD = 8
STEPS = (-1, 0, 1)
TAPS = [(a, b) for a in STEPS for b in STEPS]
LANES = 128
HALF = LANES // 2


def slot_order(peers):
    order = [0]
    mask = peers // 2
    while mask:
        order = order + [slot | mask for slot in order]
        mask //= 2
    return order


def contract(left, right, dims):
    return lax.dot_general(left, right, (dims, ((), ())), preferred_element_type=jnp.float32)


def prepare_kernel(
    embedding_hbm,
    dilation_hbm,
    kernel_hbm,
    bias_hbm,
    mixing_hbm,
    cot_hbm,
    own_ref,
    rate_ref,
    weight_ref,
    wide_ref,
    guide_ref,
    mix_ref,
    wide_bias_ref,
    rates,
    kernel_ref,
    bias_ref,
    mixing_ref,
    cot_ref,
    flat_ref,
    semaphores,
):
    pairs = (
        (kernel_hbm, kernel_ref),
        (cot_hbm, cot_ref),
        (mixing_hbm, mixing_ref),
        (bias_hbm, bias_ref),
        (dilation_hbm, rates),
        (embedding_hbm, own_ref),
    )
    copies = [pltpu.make_async_copy(*pair, semaphores.at[at]) for at, pair in enumerate(pairs)]
    for copy in copies:
        copy.start()
    filters = kernel_ref.shape[1]
    maps, rows, cols = cot_ref.shape
    weight_ref[...] = jnp.zeros_like(weight_ref)
    wide_ref[...] = jnp.zeros_like(wide_ref)
    wide_bias_ref[...] = jnp.zeros_like(wide_bias_ref)
    for copy in copies:
        copy.wait()
    lead = (0, HALF, 2 * HALF)
    side = (HALF, 0, 3 * HALF)
    for at, (a, b) in enumerate(TAPS):
        tap = kernel_ref[at]
        first = lead[a + 1]
        weight_ref[0, first : first + filters, (b + 1) * LANES : (b + 2) * LANES] = tap
        first = side[b + 1]
        weight_ref[1, first : first + filters, (a + 1) * LANES : (a + 2) * LANES] = tap
        first = (b + 1) * LANES
        wide_ref[first : first + filters, (a + 1) * LANES : (a + 2) * LANES] = tap
        first = (a + 1) * LANES + HALF
        wide_ref[first : first + filters, (b + 4) * LANES : (b + 5) * LANES] = tap
    rate_ref[0:8, :] = jnp.full((8, LANES), rates[0], jnp.int32)
    rate_ref[8:16, :] = jnp.full((8, LANES), rates[1], jnp.int32)
    wide_bias_ref[0:1, 0:filters] = bias_ref[...]
    wide_bias_ref[0:1, HALF : HALF + filters] = bias_ref[...]
    mix = 0.5 * mixing_ref[...].astype(jnp.float32)
    spare = jnp.zeros((maps, HALF - filters), jnp.float32)
    mix = jnp.concatenate([mix, spare, mix, spare], axis=1)
    mix_ref[0:maps, :] = mix
    mix_ref[maps:16, :] = jnp.zeros((16 - maps, LANES), jnp.float32)
    for t in range(maps):
        flat_ref[t * rows : (t + 1) * rows, :] = cot_ref[t].astype(jnp.float32)
    lines = [flat_ref[pl.ds(i, maps, stride=rows), :] for i in range(rows)]
    cot = jnp.concatenate(lines, axis=1).astype(jnp.bfloat16)
    mix = mix.astype(jnp.bfloat16)
    guide_ref[...] = contract(cot, mix, ((0,), (0,))).astype(jnp.bfloat16)


def contact_kernel(mix_bias_ref, mix_ref, active_ref, contact_ref):
    mix = mix_ref[...].astype(jnp.bfloat16)
    mixed = contract(mix, active_ref[...], ((1,), (1,)))
    maps = contact_ref.shape[0]
    which = lax.broadcasted_iota(jnp.int32, (8, 1), 0)
    offset = jnp.zeros((8, 1), jnp.float32)
    for t in range(maps):
        offset = jnp.where(which == t, mix_bias_ref[t], offset)
    contact_ref[...] = (mixed[0:8] + offset)[0:maps]


def local_kernel(sizes, *refs):
    peers, rows, cols, bins, filters, half = sizes
    block_refs = refs[:peers]
    rate_ref, weight_ref, wide_ref, guide_ref, bias_ref = refs[peers : peers + 5]
    active_ref, send_ref, keep_ref = refs[peers + 5 : peers + 8]
    bins_ref, pair_ref, conv_ref, center_ref, eights_ref, grad_ref, turned_ref, acc_ref, taps_ref = (
        refs[peers + 8 :]
    )
    row_rate = jnp.max(rate_ref[0:8, :])
    col_rate = jnp.max(rate_ref[8:16, :])
    row_index = lax.axis_index("row")
    col_index = lax.axis_index("col")
    row_start = row_index * rows
    col_start = col_index * cols
    core = lax.rem(row_index, 2)
    count = len(TAPS)
    bf16 = jnp.bfloat16
    f32 = jnp.float32
    extended = rows + 2 * DMAX

    bins_ref[0:PAD, :] = jnp.zeros((PAD, LANES), f32)
    bins_ref[bins + PAD : bins + 2 * PAD, :] = jnp.zeros((PAD, LANES), f32)
    for step in range(peers):
        place = pl.multiple_of(jnp.bitwise_xor(col_index, step) * cols + PAD, 8)
        bins_ref[pl.ds(place, cols), :] = 0.5 * block_refs[step][...].astype(f32)

    col_place = lax.broadcasted_iota(jnp.int32, (cols, LANES), 0) + col_start
    edge = 16
    values = []
    keeps = []
    for shift in (0, -col_rate, col_rate, -row_rate, row_rate):
        values.append(bins_ref[pl.ds(col_start + PAD + shift, cols), :].astype(bf16))
        place = col_place + shift
        keeps.append(((place >= 0) & (place < bins)).astype(f32).astype(bf16))
    for m in range(extended):
        row = bins_ref[pl.ds(row_start + PAD - DMAX + m, 1), :]
        row = jnp.broadcast_to(row, (edge, LANES)).astype(bf16)
        place = row_start - DMAX + m
        inside = ((place >= 0) & (place < bins)).astype(f32).astype(bf16)
        for slot in range(5):
            for j in range(0, cols, edge):
                piece = row + values[slot][j : j + edge]
                if slot > 0 and (j == 0 or j + edge == cols):
                    piece = piece * keeps[slot][j : j + edge]
                if m < DMAX or m >= rows + DMAX:
                    piece = piece * inside
                pair_ref[slot, m * cols + j : m * cols + j + edge, :] = piece

    def shifted_columns(first, last):
        return jnp.concatenate([pair_ref[first], pair_ref[0], pair_ref[last]], axis=1)

    lane = lax.broadcasted_iota(jnp.int32, (1, LANES), 1)
    is_mirror = lane >= HALF
    center = slice(DMAX * cols, (DMAX + rows) * cols)
    direct = contract(shifted_columns(1, 2), weight_ref[0], ((1,), (1,)))
    conv_ref[0] = direct
    mirror = contract(shifted_columns(3, 4), weight_ref[1], ((1,), (1,)))
    conv_ref[1] = mirror
    swapped = jnp.where(is_mirror, direct[center, :LANES], mirror[center, :LANES])
    center_ref[...] = pltpu.roll(swapped, HALF, 1) + bias_ref[0:1, :]

    row_keeps = []
    for q in STEPS:
        place = col_place + jnp.where(is_mirror, q * row_rate, q * col_rate)
        row_keeps.append(((place >= 0) & (place < bins)).astype(f32))
    margin = PAD * cols
    grad_ref[0:margin, :] = jnp.zeros((margin, LANES), bf16)
    grad_ref[margin + rows * cols : 2 * margin + rows * cols, :] = jnp.zeros((margin, LANES), bf16)
    last = cols - 8

    def row_step(i, col_total):
        def part(mirrored, shift, group):
            first = pl.multiple_of((DMAX + i + shift) * cols, cols)
            return conv_ref[mirrored, pl.ds(first, cols), group * LANES : (group + 1) * LANES]

        here = pl.ds(pl.multiple_of(i * cols, cols), cols)
        conv = jnp.where(is_mirror, part(1, -col_rate, 0), part(0, -row_rate, 0))
        conv = conv + center_ref[here, :]
        conv = conv + (part(0, row_rate, 1) + part(1, col_rate, 1))
        grad = jnp.where(conv > 0, guide_ref[here, :].astype(f32), 0.0)
        active_ref[here, :] = jnp.maximum(conv, 0.0).astype(bf16)
        grad_ref[pl.ds(pl.multiple_of(margin + i * cols, cols), cols), :] = grad.astype(bf16)
        inner = grad[8:16]
        for j in range(16, last, 8):
            inner = inner + grad[j : j + 8]
        for q in range(3):
            keep = row_keeps[q]
            eight = inner + grad[0:8] * keep[0:8] + grad[last:cols] * keep[last:cols]
            eights_ref[q, pl.ds(pl.multiple_of(i * 8, 8), 8), :] = eight
        return col_total + grad

    col_total = lax.fori_loop(0, rows, row_step, jnp.zeros((cols, LANES), f32), unroll=4)
    row_sums = []
    col_sums = []
    for q in range(3):
        row_sums.append(jnp.sum(eights_ref[q].reshape(rows, 8, LANES), axis=1))
        total = col_total
        for i in [*range(DMAX), *range(rows - DMAX, rows)]:
            step = STEPS[q]
            place = row_start + i + jnp.where(is_mirror, step * col_rate, step * row_rate)
            drop = ((place < 0) | (place >= bins)).astype(f32)
            total = total - grad_ref[margin + i * cols : margin + (i + 1) * cols, :].astype(f32) * drop
        col_sums.append(pltpu.roll(total, HALF, 1))

    chunks = (2 * margin + rows * cols) // LANES
    first_chunk = margin // LANES
    last_chunk = chunks - first_chunk
    blank = jnp.zeros((LANES, LANES), bf16)
    for odd in range(2):
        for chunk in range(chunks):
            at = slice(chunk * LANES, (chunk + 1) * LANES)
            if first_chunk <= chunk < last_chunk + odd:
                begin = chunk * LANES - odd * cols
                turned_ref[odd, :, at] = grad_ref[begin : begin + LANES, :].T
            else:
                turned_ref[odd, :, at] = blank

    def shifted_rows(first, rate):
        pieces = []
        for q in STEPS:
            start = (DMAX - q * rate) * cols
            odd = lax.rem(lax.rem(q * rate, 2) + 2, 2)
            start = pl.multiple_of(start + odd * cols, LANES)
            pieces.append(turned_ref[odd, first : first + filters, pl.ds(start, extended * cols)])
        return jnp.concatenate(pieces, axis=0)

    direct = contract(shifted_rows(0, row_rate), shifted_columns(1, 2), ((1,), (0,)))
    mirror = contract(shifted_rows(HALF, col_rate), shifted_columns(3, 4), ((1,), (0,)))
    for at, (a, b) in enumerate(TAPS):
        a, b = a + 1, b + 1
        taps_ref[at * filters : (at + 1) * filters, :] = (
            direct[a * filters : (a + 1) * filters, b * LANES : (b + 1) * LANES]
            + mirror[b * filters : (b + 1) * filters, a * LANES : (a + 1) * LANES]
        )

    sums = jnp.concatenate(
        [jnp.concatenate(row_sums, axis=1), jnp.concatenate(col_sums, axis=1)], axis=0
    ).astype(bf16)
    spread = contract(sums, wide_ref[...], ((1,), (0,)))
    acc_ref[...] = jnp.zeros_like(acc_ref)
    for group in range(6):
        shift = STEPS[group % 3] * (row_rate if group < 3 else col_rate)
        piece = spread[:, group * LANES : (group + 1) * LANES]
        where = pl.ds(row_start + PAD + shift, rows)
        acc_ref[where, :] = acc_ref[where, :] + piece[0:rows]
        where = pl.ds(col_start + PAD + shift, cols)
        acc_ref[where, :] = acc_ref[where, :] + piece[rows : rows + cols]

    total_rows = count * filters
    for target, which in ((keep_ref, core), (send_ref, 1 - core)):
        part = cols // 2
        for slot, step in enumerate(slot_order(peers)):
            block = jnp.bitwise_xor(col_index, step)
            first = pl.multiple_of(block * cols + which * part + PAD, 8)
            target[slot * part : (slot + 1) * part, :] = (
                0.5 * acc_ref[pl.ds(first, part), :]
            ).astype(bf16)
        first = pl.multiple_of(which * (total_rows - half), 16)
        target[peers * part : peers * part + half, :] = taps_ref[pl.ds(first, half), :].astype(bf16)


def join_kernel(half, mine_ref, other_ref, embedding_ref, taps_ref):
    core = lax.rem(lax.axis_index("row"), 2)
    total_rows = taps_ref.shape[0]
    part = embedding_ref.shape[0] // 2
    mine = mine_ref[...].astype(jnp.float32)
    other = other_ref[...].astype(jnp.float32)
    low = jnp.where(core == 0, mine, other)
    high = jnp.where(core == 0, other, mine)
    taps_ref[0 : total_rows - half, :] = low[part : part + total_rows - half]
    taps_ref[total_rows - half : total_rows, :] = high[part : part + half]
    embedding_ref[0:part, :] = low[0:part]
    embedding_ref[part : 2 * part, :] = high[0:part]


def swap(value, axis, mask):
    peers = lax.axis_size(axis)
    return lax.ppermute(value, axis, [(i, i ^ mask) for i in range(peers)])


def per_device(embedding, dilation, kernel, kernel_bias, mixing, mixing_bias, cotangent):
    f32 = jnp.float32
    bf16 = jnp.bfloat16
    filters, channels = kernel.shape[2:]
    maps, rows, cols = cotangent.shape
    peers = lax.axis_size("col")
    row_peers = lax.axis_size("row")
    bins = cols * peers
    blocks = [swap(embedding, "col", mask) for mask in range(peers - 1, 0, -1)]
    taps = len(TAPS)
    taps_rows = taps * filters
    half = (taps_rows // 2 + 15) // 16 * 16
    spots = rows * cols
    packed = half + peers * cols // 2
    vmem = pl.BlockSpec(memory_space=pltpu.VMEM)
    mib = 1024 * 1024

    def call(body, name, out_shape, inputs, scratch=(), limit=16, specs=None, flops=1000):
        return pl.pallas_call(
            body,
            out_shape=out_shape,
            in_specs=specs or [vmem] * len(inputs),
            out_specs=jax.tree.map(lambda _: vmem, out_shape),
            scratch_shapes=list(scratch),
            compiler_params=pltpu.CompilerParams(vmem_limit_bytes=limit * mib),
            cost_estimate=pl.CostEstimate(flops=flops, bytes_accessed=1000, transcendentals=0),
            name=name,
        )(*inputs)

    shape = jax.ShapeDtypeStruct
    kernels = kernel.reshape(taps, filters, channels)
    own, rates, weight, wide, guide, mix, bias = call(
        prepare_kernel,
        "prepare",
        (
            shape(embedding.shape, bf16),
            shape((16, LANES), jnp.int32),
            shape((2, 2 * LANES, 3 * LANES), bf16),
            shape((3 * LANES, 6 * LANES), bf16),
            shape((spots, LANES), bf16),
            shape((16, LANES), f32),
            shape((8, LANES), f32),
        ),
        [
            pltpu.with_memory_space_constraint(value, pltpu.HBM)
            for value in (embedding, dilation, kernels, kernel_bias[None, :], mixing, cotangent)
        ],
        scratch=(
            pltpu.SMEM((2,), jnp.int32),
            pltpu.VMEM(kernels.shape, bf16),
            pltpu.VMEM((1, filters), f32),
            pltpu.VMEM(mixing.shape, bf16),
            pltpu.VMEM(cotangent.shape, bf16),
            pltpu.VMEM((maps * rows, cols), f32),
            pltpu.SemaphoreType.DMA((6,)),
        ),
        specs=[pl.BlockSpec(memory_space=pltpu.HBM)] * 6,
        flops=4_000_000_000,
    )
    blocks = [own] + blocks[::-1]
    extended = (rows + 2 * DMAX) * cols
    padded = spots + 2 * PAD * cols
    active, send, keep = call(
        functools.partial(local_kernel, (peers, rows, cols, bins, filters, half)),
        "contact_head",
        (shape((spots, LANES), bf16), shape((packed, LANES), bf16), shape((packed, LANES), bf16)),
        (*blocks, rates, weight, wide, guide, bias),
        scratch=(
            pltpu.VMEM((bins + 2 * PAD, LANES), f32),
            pltpu.VMEM((5, extended, LANES), bf16),
            pltpu.VMEM((2, extended, 2 * LANES), f32),
            pltpu.VMEM((spots, LANES), f32),
            pltpu.VMEM((3, rows * 8, LANES), f32),
            pltpu.VMEM((padded, LANES), bf16),
            pltpu.VMEM((2, LANES, padded), bf16),
            pltpu.VMEM((bins + 2 * PAD, LANES), f32),
            pltpu.VMEM((taps_rows, LANES), f32),
        ),
        limit=24,
        flops=20_000_000_000,
    )

    total = keep + swap(send, "row", 1)
    mask = 1
    while mask < peers:
        kept = peers * (cols // 2) // (2 * mask)
        got = swap(total[kept:], "col", mask)
        total = jnp.concatenate([total[:kept] + got[:kept], total[2 * kept :] + got[kept:]], axis=0)
        mask *= 2
    contact = call(
        contact_kernel,
        "contact",
        shape((maps, spots), f32),
        (mixing_bias, mix, active),
        specs=[pl.BlockSpec(memory_space=pltpu.SMEM), vmem, vmem],
        flops=1_000_000_000,
    ).reshape(maps, rows, cols)
    total, contact = lax.optimization_barrier((total, contact))
    mask = 2
    while mask < row_peers:
        total = total + swap(total, "row", mask)
        mask *= 2
    other = swap(total, "row", 1)
    embedding_grad, kernel_grad = call(
        functools.partial(join_kernel, half),
        "join",
        (shape((cols, channels), f32), shape((taps_rows, channels), f32)),
        (total, other),
        limit=4,
    )
    return contact, embedding_grad, kernel_grad.reshape(kernel.shape)


def solution(mesh):
    return jax.shard_map(
        per_device,
        mesh=mesh,
        in_specs=(P("col", None), P(), P(), P(), P(), P(), P(None, "row", "col")),
        out_specs=(P(None, "row", "col"), P("col", None), P()),
        check_vma=False,
    )
```

```python
import functools

import jax
import jax.numpy as jnp
from jax import lax
from jax.experimental import pallas as pl
from jax.experimental.pallas import tpu as pltpu
from jax.sharding import PartitionSpec as P

DMAX = 4
PAD = 8
STEPS = (-1, 0, 1)
TAPS = [(a, b) for a in STEPS for b in STEPS]
LANES = 128
HALF = LANES // 2


def digit_groups(peers):
    groups = []
    low = 1
    while low < peers:
        size = min(4, peers // low)
        groups.append([digit * low for digit in range(size)])
        low *= size
    return groups


def slot_order(peers):
    order = [0]
    for group in digit_groups(peers)[::-1]:
        order = [digit | slot for digit in group for slot in order]
    return order


def contract(left, right, dims):
    return lax.dot_general(left, right, (dims, ((), ())), preferred_element_type=jnp.float32)


def guide_of(cot_ref, flat_ref, mix):
    maps, rows, cols = cot_ref.shape
    for t in range(maps):
        flat_ref[t * rows : (t + 1) * rows, :] = cot_ref[t].astype(jnp.float32)
    lines = [flat_ref[pl.ds(i, maps, stride=rows), :] for i in range(rows)]
    cot = jnp.concatenate(lines, axis=1).astype(jnp.bfloat16)
    return contract(cot, mix.astype(jnp.bfloat16), ((0,), (0,))).astype(jnp.bfloat16)


def prepare_kernel(
    embedding_hbm,
    dilation_hbm,
    kernel_hbm,
    bias_hbm,
    mixing_hbm,
    cot_hbm,
    own_ref,
    rate_ref,
    weight_ref,
    wide_ref,
    guide_ref,
    mix_ref,
    wide_bias_ref,
    rates,
    kernel_ref,
    bias_ref,
    mixing_ref,
    cot_ref,
    flat_ref,
    semaphores,
):
    pairs = (
        (kernel_hbm, kernel_ref),
        (cot_hbm, cot_ref),
        (mixing_hbm, mixing_ref),
        (bias_hbm, bias_ref),
        (dilation_hbm, rates),
        (embedding_hbm, own_ref),
    )
    copies = [pltpu.make_async_copy(*pair, semaphores.at[at]) for at, pair in enumerate(pairs)]
    for copy in copies:
        copy.start()
    filters = kernel_ref.shape[1]
    maps = cot_ref.shape[0]
    weight_ref[...] = jnp.zeros_like(weight_ref)
    wide_ref[...] = jnp.zeros_like(wide_ref)
    wide_bias_ref[...] = jnp.zeros_like(wide_bias_ref)
    for copy in copies:
        copy.wait()
    lead = (0, HALF, 2 * HALF)
    side = (HALF, 0, 3 * HALF)
    for at, (a, b) in enumerate(TAPS):
        tap = kernel_ref[at]
        first = lead[a + 1]
        weight_ref[0, first : first + filters, (b + 1) * LANES : (b + 2) * LANES] = tap
        first = side[b + 1]
        weight_ref[1, first : first + filters, (a + 1) * LANES : (a + 2) * LANES] = tap
        first = (b + 1) * LANES
        wide_ref[first : first + filters, (a + 1) * LANES : (a + 2) * LANES] = tap
        first = (a + 1) * LANES + HALF
        wide_ref[first : first + filters, (b + 4) * LANES : (b + 5) * LANES] = tap
    rate_ref[0:8, :] = jnp.full((8, LANES), rates[0], jnp.int32)
    rate_ref[8:16, :] = jnp.full((8, LANES), rates[1], jnp.int32)
    wide_bias_ref[0:1, 0:filters] = bias_ref[...]
    wide_bias_ref[0:1, HALF : HALF + filters] = bias_ref[...]
    mix = 0.5 * mixing_ref[...].astype(jnp.float32)
    spare = jnp.zeros((maps, HALF - filters), jnp.float32)
    mix = jnp.concatenate([mix, spare, mix, spare], axis=1)
    mix_ref[0:maps, :] = mix
    mix_ref[maps:16, :] = jnp.zeros((16 - maps, LANES), jnp.float32)
    guide_ref[...] = guide_of(cot_ref, flat_ref, mix)


def contact_kernel(mix_bias_ref, mix_ref, active_ref, contact_ref):
    mix = mix_ref[...].astype(jnp.bfloat16)
    maps, spots = contact_ref.shape
    upper = lax.axis_index("row") // (lax.axis_size("row") // 2)
    mine = pl.ds(pl.multiple_of(upper * spots, spots), spots)
    mixed = contract(mix, active_ref[mine, :], ((1,), (1,)))
    which = lax.broadcasted_iota(jnp.int32, (8, 1), 0)
    offset = jnp.zeros((8, 1), jnp.float32)
    for t in range(maps):
        offset = jnp.where(which == t, mix_bias_ref[t], offset)
    contact_ref[...] = (mixed[0:8] + offset)[0:maps]


def local_kernel(sizes, *refs):
    peers, rows, cols, bins, filters, half = sizes
    block_refs = refs[:peers]
    rate_ref, weight_ref, wide_ref, own_guide_ref, mix_ref, bias_ref, twin_cot_ref = refs[peers : peers + 7]
    active_ref, send_ref, keep_ref = refs[peers + 7 : peers + 10]
    bins_ref, pair_ref, conv_ref, center_ref, guide_ref, eights_ref = refs[peers + 10 : peers + 16]
    grad_ref, turned_ref, acc_ref, taps_ref, flat_ref = refs[peers + 16 :]
    row_rate = jnp.max(rate_ref[0:8, :])
    col_rate = jnp.max(rate_ref[8:16, :])
    row_index = lax.axis_index("row")
    col_index = lax.axis_index("col")
    split = lax.axis_size("row") // 2
    upper = row_index // split
    lower_index = lax.rem(row_index, split)
    row_starts = [lower_index * rows, (lower_index + split) * rows]
    col_start = col_index * cols
    core = lax.rem(row_index, 2)
    count = len(TAPS)
    bf16 = jnp.bfloat16
    f32 = jnp.float32
    extended = rows + 2 * DMAX
    spots = rows * cols
    blocks = range(2)

    bins_ref[0:PAD, :] = jnp.zeros((PAD, LANES), f32)
    bins_ref[bins + PAD : bins + 2 * PAD, :] = jnp.zeros((PAD, LANES), f32)
    for step in range(peers):
        place = pl.multiple_of(jnp.bitwise_xor(col_index, step) * cols + PAD, 8)
        bins_ref[pl.ds(place, cols), :] = 0.5 * block_refs[step][...].astype(f32)

    col_place = lax.broadcasted_iota(jnp.int32, (cols, LANES), 0) + col_start
    edge = 16
    values = []
    keeps = []
    for shift in (0, -col_rate, col_rate, -row_rate, row_rate):
        values.append(bins_ref[pl.ds(col_start + PAD + shift, cols), :].astype(bf16))
        place = col_place + shift
        keeps.append(((place >= 0) & (place < bins)).astype(f32).astype(bf16))
    for block in blocks:
        for m in range(extended):
            place = row_starts[block] - DMAX + m
            row = bins_ref[pl.ds(place + PAD, 1), :]
            row = jnp.broadcast_to(row, (edge, LANES)).astype(bf16)
            inside = ((place >= 0) & (place < bins)).astype(f32).astype(bf16)
            first = (block * extended + m) * cols
            for slot in range(5):
                for j in range(0, cols, edge):
                    piece = row + values[slot][j : j + edge]
                    if slot > 0 and (j == 0 or j + edge == cols):
                        piece = piece * keeps[slot][j : j + edge]
                    if m < DMAX or m >= rows + DMAX:
                        piece = piece * inside
                    pair_ref[slot, first + j : first + j + edge, :] = piece

    own = pl.ds(pl.multiple_of(upper * spots, spots), spots)
    guide_ref[own, :] = own_guide_ref[...]
    twin = pl.ds(pl.multiple_of((1 - upper) * spots, spots), spots)
    guide_ref[twin, :] = guide_of(twin_cot_ref, flat_ref, mix_ref[0 : twin_cot_ref.shape[0], :])

    def shifted_columns(first, last, block=None):
        at = slice(None) if block is None else slice(block * extended * cols, (block + 1) * extended * cols)
        return jnp.concatenate([pair_ref[first, at], pair_ref[0, at], pair_ref[last, at]], axis=1)

    lane = lax.broadcasted_iota(jnp.int32, (1, LANES), 1)
    is_mirror = lane >= HALF
    center = slice(DMAX * cols, (DMAX + rows) * cols)
    for block in blocks:
        here = slice(block * extended * cols, (block + 1) * extended * cols)
        direct = contract(shifted_columns(1, 2, block), weight_ref[0], ((1,), (1,)))
        conv_ref[0, here, :] = direct
        mirror = contract(shifted_columns(3, 4, block), weight_ref[1], ((1,), (1,)))
        conv_ref[1, here, :] = mirror
        swapped = jnp.where(is_mirror, direct[center, :LANES], mirror[center, :LANES])
        center_ref[block * spots : (block + 1) * spots, :] = pltpu.roll(swapped, HALF, 1) + bias_ref[0:1, :]

    row_keeps = []
    for q in STEPS:
        place = col_place + jnp.where(is_mirror, q * row_rate, q * col_rate)
        row_keeps.append(((place >= 0) & (place < bins)).astype(f32))
    margin = PAD * cols
    padded = 2 * margin + spots
    for block in blocks:
        for first in (block * padded, block * padded + margin + spots):
            grad_ref[first : first + margin, :] = jnp.zeros((margin, LANES), bf16)
    last = cols - 8

    def row_step(block, i, col_total):
        def part(mirrored, shift, group):
            first = pl.multiple_of((block * extended + DMAX + i + shift) * cols, cols)
            return conv_ref[mirrored, pl.ds(first, cols), group * LANES : (group + 1) * LANES]

        here = pl.ds(pl.multiple_of(block * spots + i * cols, cols), cols)
        conv = jnp.where(is_mirror, part(1, -col_rate, 0), part(0, -row_rate, 0))
        conv = conv + center_ref[here, :]
        conv = conv + (part(0, row_rate, 1) + part(1, col_rate, 1))
        grad = jnp.where(conv > 0, guide_ref[here, :].astype(f32), 0.0)
        active_ref[here, :] = jnp.maximum(conv, 0.0).astype(bf16)
        first = pl.multiple_of(block * padded + margin + i * cols, cols)
        grad_ref[pl.ds(first, cols), :] = grad.astype(bf16)
        inner = grad[8:16]
        for j in range(16, last, 8):
            inner = inner + grad[j : j + 8]
        for q in range(3):
            keep = row_keeps[q]
            eight = inner + grad[0:8] * keep[0:8] + grad[last:cols] * keep[last:cols]
            eights_ref[q, pl.ds(pl.multiple_of((block * rows + i) * 8, 8), 8), :] = eight
        return col_total + grad

    col_total = jnp.zeros((cols, LANES), f32)
    for block in blocks:
        col_total = lax.fori_loop(0, rows, functools.partial(row_step, block), col_total, unroll=4)
    row_sums = []
    col_sums = []
    for q in range(3):
        row_sums.append(jnp.sum(eights_ref[q].reshape(2 * rows, 8, LANES), axis=1))
        total = col_total
        for block in blocks:
            for i in [*range(DMAX), *range(rows - DMAX, rows)]:
                step = STEPS[q]
                place = row_starts[block] + i + jnp.where(is_mirror, step * col_rate, step * row_rate)
                drop = ((place < 0) | (place >= bins)).astype(f32)
                first = block * padded + margin + i * cols
                total = total - grad_ref[first : first + cols, :].astype(f32) * drop
        col_sums.append(pltpu.roll(total, HALF, 1))

    chunks = padded // LANES
    first_chunk = margin // LANES
    last_chunk = chunks - first_chunk
    blank = jnp.zeros((LANES, LANES), bf16)
    for block in blocks:
        for odd in range(2):
            for chunk in range(chunks):
                at = slice(block * padded + chunk * LANES, block * padded + (chunk + 1) * LANES)
                if first_chunk <= chunk < last_chunk + odd:
                    begin = block * padded + chunk * LANES - odd * cols
                    turned_ref[odd, :, at] = grad_ref[begin : begin + LANES, :].T
                else:
                    turned_ref[odd, :, at] = blank

    def shifted_rows(first, rate):
        pieces = []
        for q in STEPS:
            start = (DMAX - q * rate) * cols
            odd = lax.rem(lax.rem(q * rate, 2) + 2, 2)
            start = start + odd * cols
            wide = [
                turned_ref[
                    odd,
                    first : first + filters,
                    pl.ds(pl.multiple_of(start + block * padded, LANES), extended * cols),
                ]
                for block in blocks
            ]
            pieces.append(jnp.concatenate(wide, axis=1))
        return jnp.concatenate(pieces, axis=0)

    direct = contract(shifted_rows(0, row_rate), shifted_columns(1, 2), ((1,), (0,)))
    mirror = contract(shifted_rows(HALF, col_rate), shifted_columns(3, 4), ((1,), (0,)))
    for at, (a, b) in enumerate(TAPS):
        a, b = a + 1, b + 1
        taps_ref[at * filters : (at + 1) * filters, :] = (
            direct[a * filters : (a + 1) * filters, b * LANES : (b + 1) * LANES]
            + mirror[b * filters : (b + 1) * filters, a * LANES : (a + 1) * LANES]
        )

    sums = jnp.concatenate(
        [jnp.concatenate(row_sums, axis=1), jnp.concatenate(col_sums, axis=1)], axis=0
    ).astype(bf16)
    spread = contract(sums, wide_ref[...], ((1,), (0,)))
    acc_ref[...] = jnp.zeros_like(acc_ref)
    for group in range(6):
        shift = STEPS[group % 3] * (row_rate if group < 3 else col_rate)
        piece = spread[:, group * LANES : (group + 1) * LANES]
        for block in blocks:
            where = pl.ds(row_starts[block] + PAD + shift, rows)
            acc_ref[where, :] = acc_ref[where, :] + piece[block * rows : (block + 1) * rows]
        where = pl.ds(col_start + PAD + shift, cols)
        acc_ref[where, :] = acc_ref[where, :] + piece[2 * rows : 2 * rows + cols]

    total_rows = count * filters
    for target, which in ((keep_ref, core), (send_ref, 1 - core)):
        part = cols // 2
        for slot, step in enumerate(slot_order(peers)):
            block = jnp.bitwise_xor(col_index, step)
            first = pl.multiple_of(block * cols + which * part + PAD, 8)
            target[slot * part : (slot + 1) * part, :] = (
                0.5 * acc_ref[pl.ds(first, part), :]
            ).astype(bf16)
        first = pl.multiple_of(which * (total_rows - half), 16)
        target[peers * part : peers * part + half, :] = taps_ref[pl.ds(first, half), :].astype(bf16)


def join_kernel(half, mine_ref, other_ref, embedding_ref, taps_ref):
    core = lax.rem(lax.axis_index("row"), 2)
    total_rows = taps_ref.shape[0]
    part = embedding_ref.shape[0] // 2
    mine = mine_ref[...].astype(jnp.float32)
    other = other_ref[...].astype(jnp.float32)
    low = jnp.where(core == 0, mine, other)
    high = jnp.where(core == 0, other, mine)
    taps_ref[0 : total_rows - half, :] = low[part : part + total_rows - half]
    taps_ref[total_rows - half : total_rows, :] = high[part : part + half]
    embedding_ref[0:part, :] = low[0:part]
    embedding_ref[part : 2 * part, :] = high[0:part]


def swap(value, axis, mask):
    peers = lax.axis_size(axis)
    return lax.ppermute(value, axis, [(i, i ^ mask) for i in range(peers)])


def per_device(embedding, dilation, kernel, kernel_bias, mixing, mixing_bias, cotangent):
    f32 = jnp.float32
    bf16 = jnp.bfloat16
    filters, channels = kernel.shape[2:]
    maps, rows, cols = cotangent.shape
    peers = lax.axis_size("col")
    row_peers = lax.axis_size("row")
    bins = cols * peers
    twin_cot = swap(cotangent, "row", row_peers // 2)
    blocks = [swap(embedding, "col", mask) for mask in range(peers - 1, 0, -1)]
    taps = len(TAPS)
    taps_rows = taps * filters
    half = (taps_rows // 2 + 15) // 16 * 16
    spots = rows * cols
    packed = half + peers * cols // 2
    vmem = pl.BlockSpec(memory_space=pltpu.VMEM)
    mib = 1024 * 1024

    def call(body, name, out_shape, inputs, scratch=(), limit=16, specs=None, flops=1000):
        return pl.pallas_call(
            body,
            out_shape=out_shape,
            in_specs=specs or [vmem] * len(inputs),
            out_specs=jax.tree.map(lambda _: vmem, out_shape),
            scratch_shapes=list(scratch),
            compiler_params=pltpu.CompilerParams(vmem_limit_bytes=limit * mib),
            cost_estimate=pl.CostEstimate(flops=flops, bytes_accessed=1000, transcendentals=0),
            name=name,
        )(*inputs)

    shape = jax.ShapeDtypeStruct
    kernels = kernel.reshape(taps, filters, channels)
    own, rates, weight, wide, guide, mix, bias = call(
        prepare_kernel,
        "prepare",
        (
            shape(embedding.shape, bf16),
            shape((16, LANES), jnp.int32),
            shape((2, 2 * LANES, 3 * LANES), bf16),
            shape((3 * LANES, 6 * LANES), bf16),
            shape((spots, LANES), bf16),
            shape((16, LANES), f32),
            shape((8, LANES), f32),
        ),
        [
            pltpu.with_memory_space_constraint(value, pltpu.HBM)
            for value in (embedding, dilation, kernels, kernel_bias[None, :], mixing, cotangent)
        ],
        scratch=(
            pltpu.SMEM((2,), jnp.int32),
            pltpu.VMEM(kernels.shape, bf16),
            pltpu.VMEM((1, filters), f32),
            pltpu.VMEM(mixing.shape, bf16),
            pltpu.VMEM(cotangent.shape, bf16),
            pltpu.VMEM((maps * rows, cols), f32),
            pltpu.SemaphoreType.DMA((6,)),
        ),
        specs=[pl.BlockSpec(memory_space=pltpu.HBM)] * 6,
        flops=4_000_000_000,
    )
    blocks = [own] + blocks[::-1]
    extended = (rows + 2 * DMAX) * cols
    padded = spots + 2 * PAD * cols
    active, send, keep = call(
        functools.partial(local_kernel, (peers, rows, cols, bins, filters, half)),
        "contact_head",
        (shape((2 * spots, LANES), bf16), shape((packed, LANES), bf16), shape((packed, LANES), bf16)),
        (*blocks, rates, weight, wide, guide, mix, bias, twin_cot),
        scratch=(
            pltpu.VMEM((bins + 2 * PAD, LANES), f32),
            pltpu.VMEM((5, 2 * extended, LANES), bf16),
            pltpu.VMEM((2, 2 * extended, 2 * LANES), f32),
            pltpu.VMEM((2 * spots, LANES), f32),
            pltpu.VMEM((2 * spots, LANES), bf16),
            pltpu.VMEM((3, 2 * rows * 8, LANES), f32),
            pltpu.VMEM((2 * padded, LANES), bf16),
            pltpu.VMEM((2, LANES, 2 * padded), bf16),
            pltpu.VMEM((bins + 2 * PAD, LANES), f32),
            pltpu.VMEM((taps_rows, LANES), f32),
            pltpu.VMEM((maps * rows, cols), f32),
        ),
        limit=44,
        flops=20_000_000_000,
    )

    total = keep + swap(send, "row", 1)
    bins_left = peers * (cols // 2)
    for group in digit_groups(peers):
        each = bins_left // len(group)

        def portion(digit):
            return jnp.concatenate(
                [total[digit * each : (digit + 1) * each], total[bins_left:]], axis=0
            )

        terms = [portion(0)] + [
            swap(portion(digit), "col", group[digit]) for digit in range(1, len(group))
        ]
        terms = [term.astype(f32) for term in terms]
        while len(terms) > 1:
            terms = [left + right for left, right in zip(terms[0::2], terms[1::2])]
        total = terms[0].astype(bf16)
        bins_left = each
    contact = call(
        contact_kernel,
        "contact",
        shape((maps, spots), f32),
        (mixing_bias, mix, active),
        specs=[pl.BlockSpec(memory_space=pltpu.SMEM), vmem, vmem],
        flops=1_000_000_000,
    ).reshape(maps, rows, cols)
    total, contact = lax.optimization_barrier((total, contact))
    mask = 2
    while mask < row_peers // 2:
        total = total + swap(total, "row", mask)
        mask *= 2
    other = swap(total, "row", 1)
    embedding_grad, kernel_grad = call(
        functools.partial(join_kernel, half),
        "join",
        (shape((cols, channels), f32), shape((taps_rows, channels), f32)),
        (total, other),
        limit=4,
    )
    return contact, embedding_grad, kernel_grad.reshape(kernel.shape)


def solution(mesh):
    return jax.shard_map(
        per_device,
        mesh=mesh,
        in_specs=(P("col", None), P(), P(), P(), P(), P(), P(None, "row", "col")),
        out_specs=(P(None, "row", "col"), P("col", None), P()),
        check_vma=False,
    )
```

```python
import functools

import jax
import jax.numpy as jnp
from jax import lax
from jax.experimental import pallas as pl
from jax.experimental.pallas import tpu as pltpu
from jax.sharding import PartitionSpec as P

DMAX = 4
PAD = 8
STEPS = (-1, 0, 1)
TAPS = [(a, b) for a in STEPS for b in STEPS]
LANES = 128
HALF = LANES // 2


def digit_groups(peers):
    groups = []
    low = 1
    while low < peers:
        size = min(4, peers // low)
        groups.append([digit * low for digit in range(size)])
        low *= size
    return groups


def slot_order(peers):
    order = [0]
    for group in digit_groups(peers)[::-1]:
        order = [digit | slot for digit in group for slot in order]
    return order


def contract(left, right, dims):
    return lax.dot_general(left, right, (dims, ((), ())), preferred_element_type=jnp.float32)


def guide_of(cot_ref, flat_ref, mix):
    maps, rows, cols = cot_ref.shape
    for t in range(maps):
        flat_ref[t * rows : (t + 1) * rows, :] = cot_ref[t].astype(jnp.float32)
    lines = [flat_ref[pl.ds(i, maps, stride=rows), :] for i in range(rows)]
    cot = jnp.concatenate(lines, axis=1).astype(jnp.bfloat16)
    return contract(cot, mix.astype(jnp.bfloat16), ((0,), (0,))).astype(jnp.bfloat16)


def prepare_kernel(
    embedding_hbm,
    dilation_hbm,
    kernel_hbm,
    bias_hbm,
    mixing_hbm,
    cot_hbm,
    own_ref,
    rate_ref,
    weight_ref,
    wide_ref,
    guide_ref,
    mix_ref,
    wide_bias_ref,
    rates,
    kernel_ref,
    bias_ref,
    mixing_ref,
    cot_ref,
    flat_ref,
    semaphores,
):
    pairs = (
        (kernel_hbm, kernel_ref),
        (cot_hbm, cot_ref),
        (mixing_hbm, mixing_ref),
        (bias_hbm, bias_ref),
        (dilation_hbm, rates),
        (embedding_hbm, own_ref),
    )
    copies = [pltpu.make_async_copy(*pair, semaphores.at[at]) for at, pair in enumerate(pairs)]
    for copy in copies:
        copy.start()
    filters = kernel_ref.shape[1]
    maps = cot_ref.shape[0]
    weight_ref[...] = jnp.zeros_like(weight_ref)
    wide_ref[...] = jnp.zeros_like(wide_ref)
    wide_bias_ref[...] = jnp.zeros_like(wide_bias_ref)
    for copy in copies:
        copy.wait()
    lead = (0, HALF, 2 * HALF)
    side = (HALF, 0, 3 * HALF)
    for at, (a, b) in enumerate(TAPS):
        tap = kernel_ref[at]
        first = lead[a + 1]
        weight_ref[0, first : first + filters, (b + 1) * LANES : (b + 2) * LANES] = tap
        first = side[b + 1]
        weight_ref[1, first : first + filters, (a + 1) * LANES : (a + 2) * LANES] = tap
        first = (b + 1) * LANES
        wide_ref[first : first + filters, (a + 1) * LANES : (a + 2) * LANES] = tap
        first = (a + 1) * LANES + HALF
        wide_ref[first : first + filters, (b + 4) * LANES : (b + 5) * LANES] = tap
    rate_ref[0:8, :] = jnp.full((8, LANES), rates[0], jnp.int32)
    rate_ref[8:16, :] = jnp.full((8, LANES), rates[1], jnp.int32)
    wide_bias_ref[0:1, 0:filters] = bias_ref[...]
    wide_bias_ref[0:1, HALF : HALF + filters] = bias_ref[...]
    mix = 0.5 * mixing_ref[...].astype(jnp.float32)
    spare = jnp.zeros((maps, HALF - filters), jnp.float32)
    mix = jnp.concatenate([mix, spare, mix, spare], axis=1)
    mix_ref[0:maps, :] = mix
    mix_ref[maps:16, :] = jnp.zeros((16 - maps, LANES), jnp.float32)
    guide_ref[...] = guide_of(cot_ref, flat_ref, mix)


def contact_kernel(mix_bias_ref, mix_ref, active_ref, contact_ref):
    mix = mix_ref[...].astype(jnp.bfloat16)
    maps, spots = contact_ref.shape
    upper = lax.axis_index("row") // (lax.axis_size("row") // 2)
    mine = pl.ds(pl.multiple_of(upper * spots, spots), spots)
    mixed = contract(mix, active_ref[mine, :], ((1,), (1,)))
    which = lax.broadcasted_iota(jnp.int32, (8, 1), 0)
    offset = jnp.zeros((8, 1), jnp.float32)
    for t in range(maps):
        offset = jnp.where(which == t, mix_bias_ref[t], offset)
    contact_ref[...] = (mixed[0:8] + offset)[0:maps]


def row_blocks(rows):
    split = lax.axis_size("row") // 2
    lower = lax.rem(lax.axis_index("row"), split)
    return [lower * rows, (lower + split) * rows]


def pairs_kernel(sizes, *refs):
    peers, rows, cols, bins = sizes
    block_refs = refs[:peers]
    rate_ref, pair_ref, bins_ref, cols_ref, rows_ref = refs[peers:]
    bf16 = jnp.bfloat16
    f32 = jnp.float32
    row_rate = jnp.max(rate_ref[0:8, :])
    col_rate = jnp.max(rate_ref[8:16, :])
    row_starts = row_blocks(rows)
    col_index = lax.axis_index("col")
    col_start = col_index * cols
    extended = rows + 2 * DMAX
    edge = 16
    bins_ref[0:PAD, :] = jnp.zeros((PAD, LANES), f32)
    bins_ref[bins + PAD : bins + 2 * PAD, :] = jnp.zeros((PAD, LANES), f32)
    for step in range(peers):
        place = pl.multiple_of(jnp.bitwise_xor(col_index, step) * cols + PAD, 8)
        bins_ref[pl.ds(place, cols), :] = 0.5 * block_refs[step][...].astype(f32)
    col_place = lax.broadcasted_iota(jnp.int32, (cols, LANES), 0) + col_start
    for slot, shift in enumerate((0, -col_rate, col_rate, -row_rate, row_rate)):
        place = col_place + shift
        keep = ((place >= 0) & (place < bins)).astype(f32)
        values = bins_ref[pl.ds(col_start + PAD + shift, cols), :]
        cols_ref[slot] = values.astype(bf16)
        cols_ref[5 + slot] = keep.astype(bf16)
    for block in range(2):
        for m in range(extended):
            row = bins_ref[pl.ds(row_starts[block] - DMAX + m + PAD, 1), :]
            rows_ref[block * extended + m] = jnp.broadcast_to(row, (edge, LANES)).astype(bf16)
    for slot in range(5):
        values = [cols_ref[slot, j : j + edge, :] for j in range(0, cols, edge)]
        keeps = {j: cols_ref[5 + slot, j : j + edge, :] for j in (0, cols - edge)}
        for block in range(2):
            for m in range(extended):
                place = row_starts[block] - DMAX + m
                row = rows_ref[block * extended + m]
                inside = ((place >= 0) & (place < bins)).astype(f32).astype(bf16)
                first = (block * extended + m) * cols
                for at, j in enumerate(range(0, cols, edge)):
                    piece = row + values[at]
                    if slot > 0 and j in keeps:
                        piece = piece * keeps[j]
                    if m < DMAX or m >= rows + DMAX:
                        piece = piece * inside
                    pair_ref[slot, first + j : first + j + edge, :] = piece


def local_kernel(sizes, *refs):
    peers, rows, cols, bins, filters, half = sizes
    pair_ref, rate_ref, weight_ref, wide_ref, own_guide_ref, mix_ref, bias_ref, twin_cot_ref = refs[:8]
    active_ref, send_ref, keep_ref = refs[8:11]
    conv_ref, center_ref, guide_ref, eights_ref = refs[11:15]
    grad_ref, turned_ref, acc_ref, taps_ref, flat_ref, sums_ref = refs[15:]
    row_rate = jnp.max(rate_ref[0:8, :])
    col_rate = jnp.max(rate_ref[8:16, :])
    row_index = lax.axis_index("row")
    col_index = lax.axis_index("col")
    row_starts = row_blocks(rows)
    upper = row_index // (lax.axis_size("row") // 2)
    col_start = col_index * cols
    core = lax.rem(row_index, 2)
    count = len(TAPS)
    bf16 = jnp.bfloat16
    f32 = jnp.float32
    extended = rows + 2 * DMAX
    spots = rows * cols
    blocks = range(2)
    col_place = lax.broadcasted_iota(jnp.int32, (cols, LANES), 0) + col_start

    def shifted_columns(first, last, block):
        at = slice(block * extended * cols, (block + 1) * extended * cols)
        return jnp.concatenate([pair_ref[first, at], pair_ref[0, at], pair_ref[last, at]], axis=1)

    lane = lax.broadcasted_iota(jnp.int32, (1, LANES), 1)
    is_mirror = lane >= HALF
    center = slice(DMAX * cols, (DMAX + rows) * cols)

    def forward(block):
        here = slice(block * extended * cols, (block + 1) * extended * cols)
        direct = contract(shifted_columns(1, 2, block), weight_ref[0], ((1,), (1,)))
        conv_ref[0, here, :] = direct
        mirror = contract(shifted_columns(3, 4, block), weight_ref[1], ((1,), (1,)))
        conv_ref[1, here, :] = mirror
        swapped = jnp.where(is_mirror, direct[center, :LANES], mirror[center, :LANES])
        center_ref[block * spots : (block + 1) * spots, :] = pltpu.roll(swapped, HALF, 1) + bias_ref[0:1, :]

    row_keeps = []
    for q in STEPS:
        place = col_place + jnp.where(is_mirror, q * row_rate, q * col_rate)
        row_keeps.append(((place >= 0) & (place < bins)).astype(f32))
    margin = PAD * cols
    padded = 2 * margin + spots
    last = cols - 8

    def row_step(block, i, col_total):
        def part(mirrored, shift, group):
            first = pl.multiple_of((block * extended + DMAX + i + shift) * cols, cols)
            return conv_ref[mirrored, pl.ds(first, cols), group * LANES : (group + 1) * LANES]

        here = pl.ds(pl.multiple_of(block * spots + i * cols, cols), cols)
        conv = jnp.where(is_mirror, part(1, -col_rate, 0), part(0, -row_rate, 0))
        conv = conv + center_ref[here, :]
        conv = conv + (part(0, row_rate, 1) + part(1, col_rate, 1))
        grad = jnp.where(conv > 0, guide_ref[here, :].astype(f32), 0.0)
        active_ref[here, :] = jnp.maximum(conv, 0.0).astype(bf16)
        first = pl.multiple_of(block * padded + margin + i * cols, cols)
        grad_ref[pl.ds(first, cols), :] = grad.astype(bf16)
        inner = grad[8:16]
        for j in range(16, last, 8):
            inner = inner + grad[j : j + 8]
        for q in range(3):
            keep = row_keeps[q]
            eight = inner + grad[0:8] * keep[0:8] + grad[last:cols] * keep[last:cols]
            eights_ref[q, pl.ds(pl.multiple_of((block * rows + i) * 8, 8), 8), :] = eight
        return col_total + grad

    def row_pass(block, col_total):
        return lax.fori_loop(0, rows, functools.partial(row_step, block), col_total, unroll=4)

    chunks = padded // LANES
    first_chunk = margin // LANES
    last_chunk = chunks - first_chunk
    blank = jnp.zeros((LANES, LANES), bf16)

    def clear_margins(block):
        for first in (block * padded, block * padded + margin + spots):
            grad_ref[first : first + margin, :] = jnp.zeros((margin, LANES), bf16)
        for odd in range(2):
            for chunk in range(chunks):
                if not first_chunk <= chunk < last_chunk + odd:
                    at = slice(block * padded + chunk * LANES, block * padded + (chunk + 1) * LANES)
                    turned_ref[odd, :, at] = blank

    def turn(block):
        for odd in range(2):
            for chunk in range(first_chunk, last_chunk + odd):
                at = slice(block * padded + chunk * LANES, block * padded + (chunk + 1) * LANES)
                begin = block * padded + chunk * LANES - odd * cols
                turned_ref[odd, :, at] = grad_ref[begin : begin + LANES, :].T

    def shifted_rows(first, rate, block):
        pieces = []
        for q in STEPS:
            start = (DMAX - q * rate) * cols
            odd = lax.rem(lax.rem(q * rate, 2) + 2, 2)
            start = pl.multiple_of(start + odd * cols + block * padded, LANES)
            pieces.append(turned_ref[odd, first : first + filters, pl.ds(start, extended * cols)])
        return jnp.concatenate(pieces, axis=0)

    def backward(block):
        direct = contract(shifted_rows(0, row_rate, block), shifted_columns(1, 2, block), ((1,), (0,)))
        mirror = contract(shifted_rows(HALF, col_rate, block), shifted_columns(3, 4, block), ((1,), (0,)))
        return direct, mirror

    forward(0)
    own = pl.ds(pl.multiple_of(upper * spots, spots), spots)
    guide_ref[own, :] = own_guide_ref[...]
    twin = pl.ds(pl.multiple_of((1 - upper) * spots, spots), spots)
    guide_ref[twin, :] = guide_of(twin_cot_ref, flat_ref, mix_ref[0 : twin_cot_ref.shape[0], :])
    for block in blocks:
        clear_margins(block)
    col_total = row_pass(0, jnp.zeros((cols, LANES), f32))
    forward(1)
    turn(0)
    col_total = row_pass(1, col_total)
    turn(1)

    for q in range(3):
        totals = jnp.sum(eights_ref[q].reshape(2 * rows, 8, LANES), axis=1)
        sums_ref[0 : 2 * rows, q * LANES : (q + 1) * LANES] = totals.astype(bf16)
        total = col_total
        for block in blocks:
            for i in [*range(DMAX), *range(rows - DMAX, rows)]:
                step = STEPS[q]
                place = row_starts[block] + i + jnp.where(is_mirror, step * col_rate, step * row_rate)
                drop = ((place < 0) | (place >= bins)).astype(f32)
                first = block * padded + margin + i * cols
                total = total - grad_ref[first : first + cols, :].astype(f32) * drop
        total = pltpu.roll(total, HALF, 1)
        sums_ref[2 * rows : 2 * rows + cols, q * LANES : (q + 1) * LANES] = total.astype(bf16)
    spread = contract(sums_ref[...], wide_ref[...], ((1,), (0,)))
    acc_ref[...] = jnp.zeros_like(acc_ref)
    for group in range(6):
        shift = STEPS[group % 3] * (row_rate if group < 3 else col_rate)
        piece = spread[:, group * LANES : (group + 1) * LANES]
        for block in blocks:
            where = pl.ds(row_starts[block] + PAD + shift, rows)
            acc_ref[where, :] = acc_ref[where, :] + piece[block * rows : (block + 1) * rows]
        where = pl.ds(col_start + PAD + shift, cols)
        acc_ref[where, :] = acc_ref[where, :] + piece[2 * rows : 2 * rows + cols]
    part = cols // 2
    for target, which in ((keep_ref, core), (send_ref, 1 - core)):
        for slot, step in enumerate(slot_order(peers)):
            place = jnp.bitwise_xor(col_index, step)
            first = pl.multiple_of(place * cols + which * part + PAD, 8)
            target[slot * part : (slot + 1) * part, :] = (
                0.5 * acc_ref[pl.ds(first, part), :]
            ).astype(bf16)

    lower = backward(0)
    higher = backward(1)
    direct = lower[0] + higher[0]
    mirror = lower[1] + higher[1]
    for at, (a, b) in enumerate(TAPS):
        a, b = a + 1, b + 1
        taps_ref[at * filters : (at + 1) * filters, :] = (
            direct[a * filters : (a + 1) * filters, b * LANES : (b + 1) * LANES]
            + mirror[b * filters : (b + 1) * filters, a * LANES : (a + 1) * LANES]
        )
    total_rows = count * filters
    for target, which in ((keep_ref, core), (send_ref, 1 - core)):
        first = pl.multiple_of(which * (total_rows - half), 16)
        target[peers * part : peers * part + half, :] = taps_ref[pl.ds(first, half), :].astype(bf16)


def join_kernel(half, mine_ref, other_ref, embedding_ref, taps_ref):
    core = lax.rem(lax.axis_index("row"), 2)
    total_rows = taps_ref.shape[0]
    part = embedding_ref.shape[0] // 2
    mine = mine_ref[...].astype(jnp.float32)
    other = other_ref[...].astype(jnp.float32)
    low = jnp.where(core == 0, mine, other)
    high = jnp.where(core == 0, other, mine)
    taps_ref[0 : total_rows - half, :] = low[part : part + total_rows - half]
    taps_ref[total_rows - half : total_rows, :] = high[part : part + half]
    embedding_ref[0:part, :] = low[0:part]
    embedding_ref[part : 2 * part, :] = high[0:part]


def swap(value, axis, mask):
    peers = lax.axis_size(axis)
    return lax.ppermute(value, axis, [(i, i ^ mask) for i in range(peers)])


def per_device(embedding, dilation, kernel, kernel_bias, mixing, mixing_bias, cotangent):
    f32 = jnp.float32
    bf16 = jnp.bfloat16
    filters, channels = kernel.shape[2:]
    maps, rows, cols = cotangent.shape
    peers = lax.axis_size("col")
    row_peers = lax.axis_size("row")
    bins = cols * peers
    twin_cot = swap(cotangent, "row", row_peers // 2)
    blocks = [swap(embedding, "col", mask) for mask in range(peers - 1, 0, -1)]
    taps = len(TAPS)
    taps_rows = taps * filters
    half = (taps_rows // 2 + 15) // 16 * 16
    spots = rows * cols
    packed = half + peers * cols // 2
    vmem = pl.BlockSpec(memory_space=pltpu.VMEM)
    mib = 1024 * 1024

    def call(body, name, out_shape, inputs, scratch=(), limit=16, specs=None, flops=1000):
        return pl.pallas_call(
            body,
            out_shape=out_shape,
            in_specs=specs or [vmem] * len(inputs),
            out_specs=jax.tree.map(lambda _: vmem, out_shape),
            scratch_shapes=list(scratch),
            compiler_params=pltpu.CompilerParams(vmem_limit_bytes=limit * mib),
            cost_estimate=pl.CostEstimate(flops=flops, bytes_accessed=1000, transcendentals=0),
            name=name,
        )(*inputs)

    shape = jax.ShapeDtypeStruct
    kernels = kernel.reshape(taps, filters, channels)
    own, rates, weight, wide, guide, mix, bias = call(
        prepare_kernel,
        "prepare",
        (
            shape(embedding.shape, bf16),
            shape((16, LANES), jnp.int32),
            shape((2, 2 * LANES, 3 * LANES), bf16),
            shape((3 * LANES, 6 * LANES), bf16),
            shape((spots, LANES), bf16),
            shape((16, LANES), f32),
            shape((8, LANES), f32),
        ),
        [
            pltpu.with_memory_space_constraint(value, pltpu.HBM)
            for value in (embedding, dilation, kernels, kernel_bias[None, :], mixing, cotangent)
        ],
        scratch=(
            pltpu.SMEM((2,), jnp.int32),
            pltpu.VMEM(kernels.shape, bf16),
            pltpu.VMEM((1, filters), f32),
            pltpu.VMEM(mixing.shape, bf16),
            pltpu.VMEM(cotangent.shape, bf16),
            pltpu.VMEM((maps * rows, cols), f32),
            pltpu.SemaphoreType.DMA((6,)),
        ),
        specs=[pl.BlockSpec(memory_space=pltpu.HBM)] * 6,
        flops=4_000_000_000,
    )
    blocks = [own] + blocks[::-1]
    extended = (rows + 2 * DMAX) * cols
    padded = spots + 2 * PAD * cols
    pairs = call(
        functools.partial(pairs_kernel, (peers, rows, cols, bins)),
        "pairs",
        shape((5, 2 * extended, LANES), bf16),
        (*blocks, rates),
        scratch=(
            pltpu.VMEM((bins + 2 * PAD, LANES), f32),
            pltpu.VMEM((10, cols, LANES), bf16),
            pltpu.VMEM((2 * (rows + 2 * DMAX), 16, LANES), bf16),
        ),
        limit=12,
        flops=3_000_000_000,
    )
    active, send, keep = call(
        functools.partial(local_kernel, (peers, rows, cols, bins, filters, half)),
        "contact_head",
        (shape((2 * spots, LANES), bf16), shape((packed, LANES), bf16), shape((packed, LANES), bf16)),
        (pairs, rates, weight, wide, guide, mix, bias, twin_cot),
        scratch=(
            pltpu.VMEM((2, 2 * extended, 2 * LANES), f32),
            pltpu.VMEM((2 * spots, LANES), f32),
            pltpu.VMEM((2 * spots, LANES), bf16),
            pltpu.VMEM((3, 2 * rows * 8, LANES), f32),
            pltpu.VMEM((2 * padded, LANES), bf16),
            pltpu.VMEM((2, LANES, 2 * padded), bf16),
            pltpu.VMEM((bins + 2 * PAD, LANES), f32),
            pltpu.VMEM((taps_rows, LANES), f32),
            pltpu.VMEM((maps * rows, cols), f32),
            pltpu.VMEM((2 * rows + cols, 3 * LANES), bf16),
        ),
        limit=40,
        flops=20_000_000_000,
    )

    total = keep + swap(send, "row", 1)
    bins_left = peers * (cols // 2)
    for group in digit_groups(peers):
        each = bins_left // len(group)

        def portion(digit):
            return jnp.concatenate(
                [total[digit * each : (digit + 1) * each], total[bins_left:]], axis=0
            )

        terms = [portion(0)] + [
            swap(portion(digit), "col", group[digit]) for digit in range(1, len(group))
        ]
        terms = [term.astype(f32) for term in terms]
        while len(terms) > 1:
            terms = [left + right for left, right in zip(terms[0::2], terms[1::2])]
        total = terms[0].astype(bf16)
        bins_left = each
    contact = call(
        contact_kernel,
        "contact",
        shape((maps, spots), f32),
        (mixing_bias, mix, active),
        specs=[pl.BlockSpec(memory_space=pltpu.SMEM), vmem, vmem],
        flops=1_000_000_000,
    ).reshape(maps, rows, cols)
    total, contact = lax.optimization_barrier((total, contact))
    mask = 2
    while mask < row_peers // 2:
        total = total + swap(total, "row", mask)
        mask *= 2
    other = swap(total, "row", 1)
    embedding_grad, kernel_grad = call(
        functools.partial(join_kernel, half),
        "join",
        (shape((cols, channels), f32), shape((taps_rows, channels), f32)),
        (total, other),
        limit=4,
    )
    return contact, embedding_grad, kernel_grad.reshape(kernel.shape)


def solution(mesh):
    return jax.shard_map(
        per_device,
        mesh=mesh,
        in_specs=(P("col", None), P(), P(), P(), P(), P(), P(None, "row", "col")),
        out_specs=(P(None, "row", "col"), P("col", None), P()),
        check_vma=False,
    )
```

```python
import functools

import jax
import jax.numpy as jnp
from jax import lax
from jax.experimental import pallas as pl
from jax.experimental.pallas import tpu as pltpu
from jax.sharding import PartitionSpec as P

DMAX = 4
PAD = 8
TWIN = 2
STEPS = (-1, 0, 1)
TAPS = [(a, b) for a in STEPS for b in STEPS]
LANES = 128
HALF = LANES // 2


def digit_groups(peers):
    groups = []
    low = 1
    while low < peers:
        size = min(4, peers // low)
        groups.append([digit * low for digit in range(size)])
        low *= size
    return groups


def slot_order(peers):
    order = [0]
    for group in digit_groups(peers)[::-1]:
        order = [digit | slot for digit in group for slot in order]
    return order


def contract(left, right, dims):
    return lax.dot_general(left, right, (dims, ((), ())), preferred_element_type=jnp.float32)


def guide_of(cot_ref, flat_ref, mix):
    maps, rows, cols = cot_ref.shape
    for t in range(maps):
        flat_ref[t * rows : (t + 1) * rows, :] = cot_ref[t].astype(jnp.float32)
    lines = [flat_ref[pl.ds(i, maps, stride=rows), :] for i in range(rows)]
    cot = jnp.concatenate(lines, axis=1).astype(jnp.bfloat16)
    return contract(cot, mix.astype(jnp.bfloat16), ((0,), (0,))).astype(jnp.bfloat16)


def prepare_kernel(
    embedding_hbm,
    dilation_hbm,
    kernel_hbm,
    bias_hbm,
    mixing_hbm,
    cot_hbm,
    own_ref,
    rate_ref,
    weight_ref,
    wide_ref,
    guide_ref,
    mix_ref,
    wide_bias_ref,
    rates,
    kernel_ref,
    bias_ref,
    mixing_ref,
    cot_ref,
    flat_ref,
    semaphores,
):
    pairs = (
        (kernel_hbm, kernel_ref),
        (cot_hbm, cot_ref),
        (mixing_hbm, mixing_ref),
        (bias_hbm, bias_ref),
        (dilation_hbm, rates),
        (embedding_hbm, own_ref),
    )
    copies = [pltpu.make_async_copy(*pair, semaphores.at[at]) for at, pair in enumerate(pairs)]
    for copy in copies:
        copy.start()
    filters = kernel_ref.shape[1]
    maps = cot_ref.shape[0]
    weight_ref[...] = jnp.zeros_like(weight_ref)
    wide_ref[...] = jnp.zeros_like(wide_ref)
    wide_bias_ref[...] = jnp.zeros_like(wide_bias_ref)
    for copy in copies:
        copy.wait()
    lead = (0, HALF, 2 * HALF)
    side = (HALF, 0, 3 * HALF)
    for at, (a, b) in enumerate(TAPS):
        tap = kernel_ref[at]
        first = lead[a + 1]
        weight_ref[0, first : first + filters, (b + 1) * LANES : (b + 2) * LANES] = tap
        first = side[b + 1]
        weight_ref[1, first : first + filters, (a + 1) * LANES : (a + 2) * LANES] = tap
        first = (b + 1) * LANES
        wide_ref[first : first + filters, (a + 1) * LANES : (a + 2) * LANES] = tap
        first = (a + 1) * LANES + HALF
        wide_ref[first : first + filters, (b + 4) * LANES : (b + 5) * LANES] = tap
    rate_ref[0:8, :] = jnp.full((8, LANES), rates[0], jnp.int32)
    rate_ref[8:16, :] = jnp.full((8, LANES), rates[1], jnp.int32)
    wide_bias_ref[0:1, 0:filters] = bias_ref[...]
    wide_bias_ref[0:1, HALF : HALF + filters] = bias_ref[...]
    mix = 0.5 * mixing_ref[...].astype(jnp.float32)
    spare = jnp.zeros((maps, HALF - filters), jnp.float32)
    mix = jnp.concatenate([mix, spare, mix, spare], axis=1)
    mix_ref[0:maps, :] = mix
    mix_ref[maps:16, :] = jnp.zeros((16 - maps, LANES), jnp.float32)
    guide_ref[...] = guide_of(cot_ref, flat_ref, mix)


def contact_kernel(mix_bias_ref, mix_ref, active_ref, contact_ref):
    mix = mix_ref[...].astype(jnp.bfloat16)
    maps, spots = contact_ref.shape
    upper = upper_twin()
    mine = pl.ds(pl.multiple_of(upper * spots, spots), spots)
    mixed = contract(mix, active_ref[mine, :], ((1,), (1,)))
    which = lax.broadcasted_iota(jnp.int32, (8, 1), 0)
    offset = jnp.zeros((8, 1), jnp.float32)
    for t in range(maps):
        offset = jnp.where(which == t, mix_bias_ref[t], offset)
    contact_ref[...] = (mixed[0:8] + offset)[0:maps]


def upper_twin():
    return lax.rem(lax.axis_index("row") // TWIN, 2)


def row_blocks(rows):
    row_index = lax.axis_index("row")
    lower = row_index - TWIN * upper_twin()
    return [lower * rows, (lower + TWIN) * rows]


def pairs_kernel(sizes, *refs):
    peers, rows, cols, bins = sizes
    block_refs = refs[:peers]
    rate_ref, pair_ref, bins_ref, cols_ref, rows_ref = refs[peers:]
    bf16 = jnp.bfloat16
    f32 = jnp.float32
    row_rate = jnp.max(rate_ref[0:8, :])
    col_rate = jnp.max(rate_ref[8:16, :])
    row_starts = row_blocks(rows)
    col_index = lax.axis_index("col")
    col_start = col_index * cols
    extended = rows + 2 * DMAX
    edge = 16
    bins_ref[0:PAD, :] = jnp.zeros((PAD, LANES), f32)
    bins_ref[bins + PAD : bins + 2 * PAD, :] = jnp.zeros((PAD, LANES), f32)
    for step in range(peers):
        place = pl.multiple_of(jnp.bitwise_xor(col_index, step) * cols + PAD, 8)
        bins_ref[pl.ds(place, cols), :] = 0.5 * block_refs[step][...].astype(f32)
    col_place = lax.broadcasted_iota(jnp.int32, (cols, LANES), 0) + col_start
    for slot, shift in enumerate((0, -col_rate, col_rate, -row_rate, row_rate)):
        place = col_place + shift
        keep = ((place >= 0) & (place < bins)).astype(f32)
        values = bins_ref[pl.ds(col_start + PAD + shift, cols), :]
        cols_ref[slot] = values.astype(bf16)
        cols_ref[5 + slot] = keep.astype(bf16)
    for block in range(2):
        for m in range(extended):
            row = bins_ref[pl.ds(row_starts[block] - DMAX + m + PAD, 1), :]
            rows_ref[block * extended + m] = jnp.broadcast_to(row, (edge, LANES)).astype(bf16)
    for slot in range(5):
        values = [cols_ref[slot, j : j + edge, :] for j in range(0, cols, edge)]
        keeps = {j: cols_ref[5 + slot, j : j + edge, :] for j in (0, cols - edge)}
        for block in range(2):
            for m in range(extended):
                place = row_starts[block] - DMAX + m
                row = rows_ref[block * extended + m]
                inside = ((place >= 0) & (place < bins)).astype(f32).astype(bf16)
                first = (block * extended + m) * cols
                for at, j in enumerate(range(0, cols, edge)):
                    piece = row + values[at]
                    if slot > 0 and j in keeps:
                        piece = piece * keeps[j]
                    if m < DMAX or m >= rows + DMAX:
                        piece = piece * inside
                    pair_ref[slot, first + j : first + j + edge, :] = piece


def local_kernel(sizes, *refs):
    peers, rows, cols, bins, filters, half = sizes
    pair_ref, rate_ref, weight_ref, wide_ref, own_guide_ref, mix_ref, bias_ref, twin_cot_ref = refs[:8]
    active_ref, send_ref, keep_ref = refs[8:11]
    conv_ref, center_ref, guide_ref, eights_ref = refs[11:15]
    grad_ref, turned_ref, acc_ref, taps_ref, flat_ref, sums_ref = refs[15:]
    row_rate = jnp.max(rate_ref[0:8, :])
    col_rate = jnp.max(rate_ref[8:16, :])
    row_index = lax.axis_index("row")
    col_index = lax.axis_index("col")
    row_starts = row_blocks(rows)
    upper = upper_twin()
    col_start = col_index * cols
    core = lax.rem(row_index, 2)
    count = len(TAPS)
    bf16 = jnp.bfloat16
    f32 = jnp.float32
    extended = rows + 2 * DMAX
    spots = rows * cols
    blocks = range(2)
    col_place = lax.broadcasted_iota(jnp.int32, (cols, LANES), 0) + col_start

    def shifted_columns(first, last, block):
        at = slice(block * extended * cols, (block + 1) * extended * cols)
        return jnp.concatenate([pair_ref[first, at], pair_ref[0, at], pair_ref[last, at]], axis=1)

    lane = lax.broadcasted_iota(jnp.int32, (1, LANES), 1)
    is_mirror = lane >= HALF
    center = slice(DMAX * cols, (DMAX + rows) * cols)

    def forward(block):
        here = slice(block * extended * cols, (block + 1) * extended * cols)
        direct = contract(shifted_columns(1, 2, block), weight_ref[0], ((1,), (1,)))
        conv_ref[0, here, :] = direct
        mirror = contract(shifted_columns(3, 4, block), weight_ref[1], ((1,), (1,)))
        conv_ref[1, here, :] = mirror
        swapped = jnp.where(is_mirror, direct[center, :LANES], mirror[center, :LANES])
        center_ref[block * spots : (block + 1) * spots, :] = pltpu.roll(swapped, HALF, 1) + bias_ref[0:1, :]

    row_keeps = []
    for q in STEPS:
        place = col_place + jnp.where(is_mirror, q * row_rate, q * col_rate)
        row_keeps.append(((place >= 0) & (place < bins)).astype(f32))
    margin = PAD * cols
    padded = 2 * margin + spots
    last = cols - 8

    def row_step(block, i, col_total):
        def part(mirrored, shift, group):
            first = pl.multiple_of((block * extended + DMAX + i + shift) * cols, cols)
            return conv_ref[mirrored, pl.ds(first, cols), group * LANES : (group + 1) * LANES]

        here = pl.ds(pl.multiple_of(block * spots + i * cols, cols), cols)
        conv = jnp.where(is_mirror, part(1, -col_rate, 0), part(0, -row_rate, 0))
        conv = conv + center_ref[here, :]
        conv = conv + (part(0, row_rate, 1) + part(1, col_rate, 1))
        grad = jnp.where(conv > 0, guide_ref[here, :].astype(f32), 0.0)
        active_ref[here, :] = jnp.maximum(conv, 0.0).astype(bf16)
        first = pl.multiple_of(block * padded + margin + i * cols, cols)
        grad_ref[pl.ds(first, cols), :] = grad.astype(bf16)
        inner = grad[8:16]
        for j in range(16, last, 8):
            inner = inner + grad[j : j + 8]
        for q in range(3):
            keep = row_keeps[q]
            eight = inner + grad[0:8] * keep[0:8] + grad[last:cols] * keep[last:cols]
            eights_ref[q, pl.ds(pl.multiple_of((block * rows + i) * 8, 8), 8), :] = eight
        return col_total + grad

    def row_pass(block, col_total):
        return lax.fori_loop(0, rows, functools.partial(row_step, block), col_total, unroll=4)

    chunks = padded // LANES
    first_chunk = margin // LANES
    last_chunk = chunks - first_chunk
    blank = jnp.zeros((LANES, LANES), bf16)

    def clear_margins(block):
        for first in (block * padded, block * padded + margin + spots):
            grad_ref[first : first + margin, :] = jnp.zeros((margin, LANES), bf16)
        for odd in range(2):
            for chunk in range(chunks):
                if not first_chunk <= chunk < last_chunk + odd:
                    at = slice(block * padded + chunk * LANES, block * padded + (chunk + 1) * LANES)
                    turned_ref[odd, :, at] = blank

    def turn(block):
        for odd in range(2):
            for chunk in range(first_chunk, last_chunk + odd):
                at = slice(block * padded + chunk * LANES, block * padded + (chunk + 1) * LANES)
                begin = block * padded + chunk * LANES - odd * cols
                turned_ref[odd, :, at] = grad_ref[begin : begin + LANES, :].T

    def shifted_rows(first, rate, block):
        pieces = []
        for q in STEPS:
            start = (DMAX - q * rate) * cols
            odd = lax.rem(lax.rem(q * rate, 2) + 2, 2)
            start = pl.multiple_of(start + odd * cols + block * padded, LANES)
            pieces.append(turned_ref[odd, first : first + filters, pl.ds(start, extended * cols)])
        return jnp.concatenate(pieces, axis=0)

    def backward(block):
        direct = contract(shifted_rows(0, row_rate, block), shifted_columns(1, 2, block), ((1,), (0,)))
        mirror = contract(shifted_rows(HALF, col_rate, block), shifted_columns(3, 4, block), ((1,), (0,)))
        return direct, mirror

    forward(0)
    own = pl.ds(pl.multiple_of(upper * spots, spots), spots)
    guide_ref[own, :] = own_guide_ref[...]
    twin = pl.ds(pl.multiple_of((1 - upper) * spots, spots), spots)
    guide_ref[twin, :] = guide_of(twin_cot_ref, flat_ref, mix_ref[0 : twin_cot_ref.shape[0], :])
    for block in blocks:
        clear_margins(block)
    col_total = row_pass(0, jnp.zeros((cols, LANES), f32))
    forward(1)
    turn(0)
    col_total = row_pass(1, col_total)
    turn(1)

    for q in range(3):
        totals = jnp.sum(eights_ref[q].reshape(2 * rows, 8, LANES), axis=1)
        sums_ref[0 : 2 * rows, q * LANES : (q + 1) * LANES] = totals.astype(bf16)
        total = col_total
        for block in blocks:
            for i in [*range(DMAX), *range(rows - DMAX, rows)]:
                step = STEPS[q]
                place = row_starts[block] + i + jnp.where(is_mirror, step * col_rate, step * row_rate)
                drop = ((place < 0) | (place >= bins)).astype(f32)
                first = block * padded + margin + i * cols
                total = total - grad_ref[first : first + cols, :].astype(f32) * drop
        total = pltpu.roll(total, HALF, 1)
        sums_ref[2 * rows : 2 * rows + cols, q * LANES : (q + 1) * LANES] = total.astype(bf16)
    spread = contract(sums_ref[...], wide_ref[...], ((1,), (0,)))
    acc_ref[...] = jnp.zeros_like(acc_ref)
    for group in range(6):
        shift = STEPS[group % 3] * (row_rate if group < 3 else col_rate)
        piece = spread[:, group * LANES : (group + 1) * LANES]
        for block in blocks:
            where = pl.ds(row_starts[block] + PAD + shift, rows)
            acc_ref[where, :] = acc_ref[where, :] + piece[block * rows : (block + 1) * rows]
        where = pl.ds(col_start + PAD + shift, cols)
        acc_ref[where, :] = acc_ref[where, :] + piece[2 * rows : 2 * rows + cols]
    part = cols // 2
    for target, which in ((keep_ref, core), (send_ref, 1 - core)):
        for slot, step in enumerate(slot_order(peers)):
            place = jnp.bitwise_xor(col_index, step)
            first = pl.multiple_of(place * cols + which * part + PAD, 8)
            target[slot * part : (slot + 1) * part, :] = (
                0.5 * acc_ref[pl.ds(first, part), :]
            ).astype(bf16)

    lower = backward(0)
    higher = backward(1)
    direct = lower[0] + higher[0]
    mirror = lower[1] + higher[1]
    for at, (a, b) in enumerate(TAPS):
        a, b = a + 1, b + 1
        taps_ref[at * filters : (at + 1) * filters, :] = (
            direct[a * filters : (a + 1) * filters, b * LANES : (b + 1) * LANES]
            + mirror[b * filters : (b + 1) * filters, a * LANES : (a + 1) * LANES]
        )
    total_rows = count * filters
    for target, which in ((keep_ref, core), (send_ref, 1 - core)):
        first = pl.multiple_of(which * (total_rows - half), 16)
        target[peers * part : peers * part + half, :] = taps_ref[pl.ds(first, half), :].astype(bf16)


def join_kernel(half, mine_ref, other_ref, embedding_ref, taps_ref):
    core = lax.rem(lax.axis_index("row"), 2)
    total_rows = taps_ref.shape[0]
    part = embedding_ref.shape[0] // 2
    mine = mine_ref[...].astype(jnp.float32)
    other = other_ref[...].astype(jnp.float32)
    low = jnp.where(core == 0, mine, other)
    high = jnp.where(core == 0, other, mine)
    taps_ref[0 : total_rows - half, :] = low[part : part + total_rows - half]
    taps_ref[total_rows - half : total_rows, :] = high[part : part + half]
    embedding_ref[0:part, :] = low[0:part]
    embedding_ref[part : 2 * part, :] = high[0:part]


def swap(value, axis, mask):
    peers = lax.axis_size(axis)
    return lax.ppermute(value, axis, [(i, i ^ mask) for i in range(peers)])


def per_device(embedding, dilation, kernel, kernel_bias, mixing, mixing_bias, cotangent):
    f32 = jnp.float32
    bf16 = jnp.bfloat16
    filters, channels = kernel.shape[2:]
    maps, rows, cols = cotangent.shape
    peers = lax.axis_size("col")
    row_peers = lax.axis_size("row")
    bins = cols * peers
    twin_cot = swap(cotangent, "row", TWIN)
    blocks = [swap(embedding, "col", mask) for mask in range(peers - 1, 0, -1)]
    taps = len(TAPS)
    taps_rows = taps * filters
    half = (taps_rows // 2 + 15) // 16 * 16
    spots = rows * cols
    packed = half + peers * cols // 2
    vmem = pl.BlockSpec(memory_space=pltpu.VMEM)
    mib = 1024 * 1024

    def call(body, name, out_shape, inputs, scratch=(), limit=16, specs=None, flops=1000):
        return pl.pallas_call(
            body,
            out_shape=out_shape,
            in_specs=specs or [vmem] * len(inputs),
            out_specs=jax.tree.map(lambda _: vmem, out_shape),
            scratch_shapes=list(scratch),
            compiler_params=pltpu.CompilerParams(vmem_limit_bytes=limit * mib),
            cost_estimate=pl.CostEstimate(flops=flops, bytes_accessed=1000, transcendentals=0),
            name=name,
        )(*inputs)

    shape = jax.ShapeDtypeStruct
    kernels = kernel.reshape(taps, filters, channels)
    own, rates, weight, wide, guide, mix, bias = call(
        prepare_kernel,
        "prepare",
        (
            shape(embedding.shape, bf16),
            shape((16, LANES), jnp.int32),
            shape((2, 2 * LANES, 3 * LANES), bf16),
            shape((3 * LANES, 6 * LANES), bf16),
            shape((spots, LANES), bf16),
            shape((16, LANES), f32),
            shape((8, LANES), f32),
        ),
        [
            pltpu.with_memory_space_constraint(value, pltpu.HBM)
            for value in (embedding, dilation, kernels, kernel_bias[None, :], mixing, cotangent)
        ],
        scratch=(
            pltpu.SMEM((2,), jnp.int32),
            pltpu.VMEM(kernels.shape, bf16),
            pltpu.VMEM((1, filters), f32),
            pltpu.VMEM(mixing.shape, bf16),
            pltpu.VMEM(cotangent.shape, bf16),
            pltpu.VMEM((maps * rows, cols), f32),
            pltpu.SemaphoreType.DMA((6,)),
        ),
        specs=[pl.BlockSpec(memory_space=pltpu.HBM)] * 6,
        flops=4_000_000_000,
    )
    blocks = [own] + blocks[::-1]
    extended = (rows + 2 * DMAX) * cols
    padded = spots + 2 * PAD * cols
    pairs = call(
        functools.partial(pairs_kernel, (peers, rows, cols, bins)),
        "pairs",
        shape((5, 2 * extended, LANES), bf16),
        (*blocks, rates),
        scratch=(
            pltpu.VMEM((bins + 2 * PAD, LANES), f32),
            pltpu.VMEM((10, cols, LANES), bf16),
            pltpu.VMEM((2 * (rows + 2 * DMAX), 16, LANES), bf16),
        ),
        limit=12,
        flops=3_000_000_000,
    )
    active, send, keep = call(
        functools.partial(local_kernel, (peers, rows, cols, bins, filters, half)),
        "contact_head",
        (shape((2 * spots, LANES), bf16), shape((packed, LANES), bf16), shape((packed, LANES), bf16)),
        (pairs, rates, weight, wide, guide, mix, bias, twin_cot),
        scratch=(
            pltpu.VMEM((2, 2 * extended, 2 * LANES), f32),
            pltpu.VMEM((2 * spots, LANES), f32),
            pltpu.VMEM((2 * spots, LANES), bf16),
            pltpu.VMEM((3, 2 * rows * 8, LANES), f32),
            pltpu.VMEM((2 * padded, LANES), bf16),
            pltpu.VMEM((2, LANES, 2 * padded), bf16),
            pltpu.VMEM((bins + 2 * PAD, LANES), f32),
            pltpu.VMEM((taps_rows, LANES), f32),
            pltpu.VMEM((maps * rows, cols), f32),
            pltpu.VMEM((2 * rows + cols, 3 * LANES), bf16),
        ),
        limit=40,
        flops=20_000_000_000,
    )

    total = keep + swap(send, "row", 1)
    bins_left = peers * (cols // 2)
    for group in digit_groups(peers):
        each = bins_left // len(group)

        def portion(digit):
            return jnp.concatenate(
                [total[digit * each : (digit + 1) * each], total[bins_left:]], axis=0
            )

        terms = [portion(0)] + [
            swap(portion(digit), "col", group[digit]) for digit in range(1, len(group))
        ]
        terms = [term.astype(f32) for term in terms]
        while len(terms) > 1:
            terms = [left + right for left, right in zip(terms[0::2], terms[1::2])]
        total = terms[0].astype(bf16)
        bins_left = each
    contact = call(
        contact_kernel,
        "contact",
        shape((maps, spots), f32),
        (mixing_bias, mix, active),
        specs=[pl.BlockSpec(memory_space=pltpu.SMEM), vmem, vmem],
        flops=1_000_000_000,
    ).reshape(maps, rows, cols)
    total, contact = lax.optimization_barrier((total, contact))
    mask = 2 * TWIN
    while mask < row_peers:
        total = total + swap(total, "row", mask)
        mask *= 2
    other = swap(total, "row", 1)
    embedding_grad, kernel_grad = call(
        functools.partial(join_kernel, half),
        "join",
        (shape((cols, channels), f32), shape((taps_rows, channels), f32)),
        (total, other),
        limit=4,
    )
    return contact, embedding_grad, kernel_grad.reshape(kernel.shape)


def solution(mesh):
    return jax.shard_map(
        per_device,
        mesh=mesh,
        in_specs=(P("col", None), P(), P(), P(), P(), P(), P(None, "row", "col")),
        out_specs=(P(None, "row", "col"), P("col", None), P()),
        check_vma=False,
    )
```
